32 devices in a mesh: dom: 8 (over z, x), en: 4 (over y, core).
Axes of the slice: x: 2, y: 2, z: 4, core: 2. Of those that a mesh axis runs over, the one named last changes fastest.
Arguments:
- single_site: bfloat16 [4, 2048, 1024], P('en', 'dom'), may hold values from -1 to 1
- coupling: bfloat16 [16, 4, 4225], P('dom'), may hold values from -0.75 to 0.75
- angular: bfloat16 [4, 1024], replicated, may hold values from -1 to 1
- phases: float32 [4, 4], P('en'), may hold values from 0.22 to 0.38
- contour: float32 [4], P('en'), may hold values from 1 to 4
- radial: bfloat16 [4, 1024, 3136], P('en'), may hold values from -0.1875 to 0.1875
- neighbours: int32 [8, 2, 65], replicated, may hold values from 0 to 2047, as said below
- owner_row: int32 [2048], replicated, may hold values from 0 to 2047, as said below
- old_potential: float32 [16, 3136], P('dom'), may hold values from -1 to 1
Outputs:
- potential: float32 [16, 3136], P('dom')
The draws below stay inside these ranges and needn't reach their ends.
Inputs may be any that keep to these rules, and one draw needn't show every extreme that they name: `neighbours`: each zone lists distinct atoms; no atom appears twice among the 130 entries of one domain's zones. Atom a lies in row owner_row[a], which belongs to domain owner_row[a] // 256; every zone's central atom belongs to the zone's own domain, and every listed atom to a domain within 2 of it along dom, counted cyclically. At most 48 entries of one domain's zones belong to any one domain; the domain itself holds exactly 48 of them, and so does one other domain. `owner_row`: A permutation of the atoms.
All inputs are finite; a program needn't handle non-finite values.
Results may differ from the reference program's by a relative error of at most 0.0029.
Values may be sent and summed in bfloat16 or wider, within the bound.
No kernel may reach another device: no remote copies, remote signals or barrier semaphores. Data moves between devices by JAX's collectives and lax.ppermute only.
A program may use at most 64 MiB of HBM per device.

```python
import math
import jax
import jax.numpy as jnp
from jax import lax

BLK = 32
ZA = 65
TERMS = 4
KR = 3136
ZONES_DEV = 2
A_DOM = 256
REACH = 2
ITERS = 2
CAP = 48
ATOMS = 2048
ZONES = 16
ENERGIES = 4


def zone_layout(key):
    folded = jax.random.fold_in(key, 7)
    subkeys = jax.random.split(folded, 5)
    domain_count = ATOMS // A_DOM
    offset_count = 2 * REACH + 1
    slot_total = offset_count * CAP
    entry_total = ZA * ZONES_DEV
    owner_rows = jax.random.permutation(subkeys[0], ATOMS).astype(jnp.int32)
    atom_of_row = jnp.argsort(owner_rows).astype(jnp.int32)
    noise_bits = jax.random.randint(subkeys[1], (domain_count, offset_count, A_DOM), 0, 2 ** 18)
    picked = jnp.argsort(noise_bits * A_DOM + jnp.arange(A_DOM, dtype=jnp.int32), axis=-1)[..., :CAP].astype(jnp.int32)
    heavy_offset = jax.random.randint(subkeys[2], (domain_count,), 0, 2 * REACH)
    heavy_offset = heavy_offset + (heavy_offset >= REACH).astype(jnp.int32)
    slot_ids = jnp.arange(slot_total, dtype=jnp.int32)
    slot_offset = slot_ids // CAP
    priority = jnp.where(slot_offset[None, :] == REACH, 2, jnp.where(slot_offset[None, :] == heavy_offset[:, None], 1, 0))
    scores = jax.random.randint(subkeys[3], (domain_count, slot_total), 0, 2 ** 20) * slot_total + slot_ids[None, :] + priority * 2 ** 29
    chosen = jnp.argsort(-scores, axis=-1)[:, :entry_total].astype(jnp.int32)
    centres = chosen[:, :ZONES_DEV]
    others = chosen[:, ZONES_DEV:]
    other_count = entry_total - ZONES_DEV
    shuffle_keys = jax.random.randint(subkeys[4], (domain_count, other_count), 0, 2 ** 20) * other_count + jnp.arange(other_count, dtype=jnp.int32)[None, :]
    others = jnp.take_along_axis(others, jnp.argsort(shuffle_keys, axis=-1), axis=-1).reshape(domain_count, ZONES_DEV, ZA - 1)
    zone_slots = jnp.concatenate([centres[:, :, None], others], axis=-1)
    offset_index = zone_slots // CAP
    slot_place = zone_slots % CAP
    domain_ids = jnp.arange(domain_count, dtype=jnp.int32)[:, None, None]
    owners = (domain_ids + offset_index - REACH) % domain_count
    local_row = picked[domain_ids, offset_index, slot_place]
    entry_rows = owners * A_DOM + local_row
    return (atom_of_row[entry_rows].astype(jnp.int32), owner_rows)


def draw_neighbours(key, part):
    return zone_layout(key)[0]


def draw_owner_row(key, part):
    return zone_layout(key)[1]


def block_levels(key, shape, cuts, least, high):
    gain = 1.0
    for axis_at, shards_of in cuts:
        draws = jax.random.uniform(jax.random.fold_in(jax.random.fold_in(key, 6), axis_at), (shards_of,), jnp.float32, least / len(cuts), high / len(cuts))
        gain = gain * jnp.repeat(jnp.exp(draws), shape[axis_at] // shards_of).reshape((-1,) + (1,) * (len(shape) - 1 - axis_at))
    return gain


def noise(stream_key, dims, width, most, cuts=(), held_as=jnp.bfloat16):
    values = width * jax.random.normal(stream_key, dims, jnp.float32)
    if cuts:
        values = values * block_levels(stream_key, dims, cuts, -0.22, 0.18)
    return jnp.clip(values, -most, most).astype(held_as)


def setup_inputs(seed: int = 0) -> dict:
    arg_keys = jax.random.split(jax.random.key(seed), 10)
    return {
        "single_site": noise(arg_keys[0], (ENERGIES, ATOMS, BLK * BLK), BLK ** -0.5, 1.0, ((0, 4), (1, 8))),
        "coupling": noise(arg_keys[1], (ZONES, TERMS, ZA * ZA), ZA ** -0.5, 0.75, ((0, 8),)),
        "angular": noise(arg_keys[2], (TERMS, BLK * BLK), BLK ** -0.5, 1.0),
        "phases": jnp.clip(0.22 + 0.16 * jax.random.uniform(arg_keys[3], (ENERGIES, TERMS), jnp.float32) ** block_levels(arg_keys[3], (ENERGIES, TERMS), ((0, 4),), -0.2, 0.2), 0.22, 0.38),
        "contour": jnp.clip(jnp.exp(math.log(4.0) - 1.3862944 * jax.random.uniform(arg_keys[4], (ENERGIES,), jnp.float32) ** block_levels(arg_keys[4], (ENERGIES,), ((0, 4),), -0.2, 0.2)), 1.0, 4.0),
        "radial": noise(arg_keys[5], (ENERGIES, BLK * BLK, KR), (BLK * BLK) ** -0.5, 0.1875, ((0, 4),)),
        "neighbours": draw_neighbours(jax.random.fold_in(arg_keys[9], 71), 0),
        "owner_row": draw_owner_row(jax.random.fold_in(arg_keys[9], 71), 0),
        "old_potential": jnp.clip(jax.random.uniform(arg_keys[8], (ZONES, KR), jnp.float32, -1.0, 1.0) * block_levels(arg_keys[8], (ZONES, KR), ((0, 8),), -0.4, 0.0), -1.0, 1.0),
    }


def rounded(values):
    return lax.optimization_barrier(values.astype(jnp.bfloat16)).astype(jnp.float32)

def reference(single_site, coupling, angular, phases, contour, radial, neighbours, owner_row, old_potential):
    entry_rows = owner_row[neighbours.reshape(-1)].reshape(ZONES, ZA).astype(jnp.int32)
    tables = angular.astype(jnp.float32).reshape(TERMS, BLK, BLK)
    couple32 = coupling.astype(jnp.float32).reshape(ZONES, TERMS, ZA, ZA)

    def one_energy(energy_index):
        block_table = single_site[energy_index].astype(jnp.float32)
        site_blocks = block_table[entry_rows].reshape(ZONES, ZA, BLK, BLK)
        scaled = phases[energy_index][None, :, None, None] * couple32
        scaled = rounded(scaled.transpose(0, 2, 1, 3)).reshape(ZONES, ZA, TERMS * ZA)
        start = jnp.zeros((ZONES, ZA, BLK, BLK), jnp.float32).at[:, 0].set(site_blocks[:, 0])
        iterate = start
        for repeat in range(ITERS):
            sweep_in = rounded(iterate)
            spread = rounded(jnp.einsum('qab,zjbc->zqjac', tables, sweep_in))
            spread = spread.reshape(ZONES, TERMS * ZA, BLK * BLK)
            field_sum = jnp.einsum('zik,zkm->zim', scaled, spread)
            field_half = rounded(field_sum).reshape(ZONES, ZA, BLK, BLK)
            iterate = start + jnp.einsum('ziab,zibc->ziac', site_blocks, field_half)
        central = rounded(iterate[:, 0]).reshape(ZONES, BLK * BLK)
        return contour[energy_index] * jnp.dot(central, radial[energy_index].astype(jnp.float32))
    energy_parts = lax.map(one_energy, jnp.arange(ENERGIES, dtype=jnp.int32))
    density = lax.optimization_barrier(jnp.sum(energy_parts, axis=0))
    return 0.5 * old_potential + 0.5 * density / jnp.sqrt(1.0 + density * density)
```

```python
import functools
import math

import jax
import jax.numpy as jnp
from jax import lax
from jax.experimental import pallas as pl
from jax.experimental.pallas import tpu as pltpu
from jax.sharding import PartitionSpec as P

REACH = 2
CAP = 48
LANES = 128
SUBS = 8
OFFSETS = tuple(offset for offset in range(-REACH, REACH + 1) if offset != 0)
F32 = jnp.float32
BF16 = jnp.bfloat16


def matmul(a, b, dims=((1,), (0,))):
    return lax.dot_general(a, b, (dims, ((), ())), preferred_element_type=F32)


def iota(shape, axis):
    return lax.broadcasted_iota(jnp.int32, shape, axis)


def ones_where(mask):
    return jnp.where(mask, 1.0, 0.0).astype(BF16)


def split(x):
    high = x.astype(BF16)
    return high, (x - high.astype(F32)).astype(BF16)


def load_lists(nbr_ref, pad_ref, targets):
    zones, places = nbr_ref.shape[1:]
    pad_ref[...] = jnp.full(pad_ref.shape, -1, jnp.int32)
    for k, target in enumerate(targets):
        pad_ref[k * zones : (k + 1) * zones, 0:places] = nbr_ref[target]
    return jnp.concatenate(
        [pad_ref[r : r + 1, :] for r in range(len(targets) * zones)], axis=1
    )


def resolve(atoms, table_ref, owned):
    table = table_ref[...]
    if owned & (owned - 1) == 0:
        shift = owned.bit_length() - 1
        domain, local = table >> shift, table & (owned - 1)
    else:
        domain, local = table // owned, table % owned
    both = jnp.concatenate([domain, local], axis=1).astype(F32).astype(BF16)
    width = atoms.shape[1]
    row_hot = ones_where(iota((table.shape[0], width), 0) == (atoms >> 7))
    picked = matmul(both, row_hot, ((0,), (0,)))
    lane_hot = iota((LANES, width), 0) == (atoms & (LANES - 1))
    found = [
        jnp.sum(jnp.where(lane_hot, picked[i * LANES : (i + 1) * LANES], 0.0), axis=0, keepdims=True)
        for i in range(2)
    ]
    return jnp.where(atoms < 0, -1.0, found[0]), found[1]


def slot_hot(masks):
    width = masks[0].shape[1]
    rows = jnp.concatenate(
        [jnp.where(mask, 1.0, 0.0) for mask in masks]
        + [jnp.zeros((SUBS - len(masks), width), F32)],
        axis=0,
    ).astype(BF16)
    earlier = ones_where(iota((width, width), 0) < iota((width, width), 1))
    rank = matmul(rows, earlier)
    slots = iota((CAP, width), 0).astype(F32)
    return [
        ones_where((rank[k : k + 1] == slots) & mask) for k, mask in enumerate(masks)
    ]


def pack_kernel(axis, nbr_ref, table_ref, site_ref, *refs):
    pack_refs, pad_ref = refs[:-1], refs[-1]
    count = nbr_ref.shape[0]
    owned = site_ref.shape[0]
    me = lax.axis_index(axis)
    atoms = load_lists(nbr_ref, pad_ref, [lax.rem(me + o + count, count) for o in OFFSETS])
    domain, local = resolve(atoms, table_ref, owned)
    width = atoms.shape[1] // len(OFFSETS)
    mine = domain == me.astype(F32)
    spans = [slice(k * width, (k + 1) * width) for k in range(len(OFFSETS))]
    hots = slot_hot([mine[:, s] for s in spans])
    rows = iota((owned, width), 0).astype(F32)
    chosen = [
        matmul(hot, ones_where(local[:, s] == rows), ((1,), (1,))).astype(BF16)
        for hot, s in zip(hots, spans)
    ]
    packed = matmul(jnp.concatenate(chosen, axis=0), site_ref[...]).astype(BF16)
    for k, pack_ref in enumerate(pack_refs):
        pack_ref[...] = packed[k * CAP : (k + 1) * CAP]


def fold_matrix():
    return ones_where(
        (iota((LANES, LANES), 0) % 32) == (iota((LANES, LANES), 1) % 32)
    )


def block_mask():
    return (iota((LANES, LANES), 0) // 32) == (iota((LANES, LANES), 1) // 32)


def prepare_kernel(
    axis,
    nbr_ref, table_ref, site_ref, first_ref, last_ref, phase_ref, angular_ref,
    slot_ref, own_ref, chain_ref, spread_ref, start_ref, centre_ref,
    pad_ref, scaled_ref, grid_ref,
):
    count, zones, places = nbr_ref.shape
    owned = site_ref.shape[0]
    terms = angular_ref.shape[0]
    groups = angular_ref.shape[1] // LANES
    me = lax.axis_index(axis)
    atoms = load_lists(nbr_ref, pad_ref, [me])
    domain, local = resolve(atoms, table_ref, owned)
    width = atoms.shape[1]
    hots = slot_hot(
        [domain == lax.rem(me - o + count, count).astype(F32) for o in OFFSETS]
    )
    scaled_ref[...] = jnp.zeros(scaled_ref.shape, F32)
    for z in range(zones):
        for q in range(terms):
            phase = phase_ref[0, q]
            for half, ref in enumerate((first_ref, last_ref)):
                row = (phase * ref[z, q : q + 1, :].astype(F32)).astype(BF16)
                at = half * zones * SUBS + z * SUBS + q
                scaled_ref[at : at + 1, 0:places] = row.astype(F32)
    coefs = []
    for z in range(zones):
        to_first = scaled_ref[z * SUBS : (z + 1) * SUBS, :]
        at = (zones + z) * SUBS
        rows = jnp.concatenate(
            [scaled_ref[at + p : at + p + 1, :] * to_first for p in range(terms)], axis=0
        )
        blank = jnp.zeros(rows.shape, F32)
        coefs.append(
            jnp.concatenate([rows if y == z else blank for y in range(zones)], axis=1)
        )
    high, low = split(jnp.concatenate(coefs, axis=0))
    size = high.shape[0]
    both = jnp.concatenate([high, low], axis=0)
    slot_ref[...] = matmul(both, jnp.concatenate(hots, axis=0), ((1,), (1,))).astype(BF16)
    centres = ones_where(
        iota((2 * SUBS, width), 1) == iota((2 * SUBS, width), 0) * LANES
    )
    own_hot = ones_where(
        (local == iota((owned, width), 0).astype(F32)) & (domain == me.astype(F32))
    )
    own_coefs = matmul(jnp.concatenate([both, centres], axis=0), own_hot, ((1,), (1,)))
    own = matmul(own_coefs.astype(BF16), site_ref[...])
    own_ref[...] = own[:size] + own[size : 2 * size]
    centre = own[2 * size : 2 * size + zones]

    for g in range(groups):
        at = slice(g * LANES, (g + 1) * LANES)
        for q in range(terms):
            grid_ref[g : g + 1, q * LANES : (q + 1) * LANES] = angular_ref[q : q + 1, at].astype(F32)
        for z in range(zones):
            m = terms + z
            grid_ref[g : g + 1, m * LANES : (m + 1) * LANES] = centre[z : z + 1, at]
    grid = grid_ref[...]
    for z in range(zones):
        m = terms + z
        centre_ref[z * groups : (z + 1) * groups, :] = grid[:, m * LANES : (m + 1) * LANES]
        start_ref[z * groups * SUBS : (z + 1) * groups * SUBS, :] = jnp.concatenate(
            [
                scaled_ref[z * SUBS : (z + 1) * SUBS, 0:1] * grid[g : g + 1, m * LANES : (m + 1) * LANES]
                for g in range(groups)
            ],
            axis=0,
        )
    repeat = ones_where(iota((32, groups), 0) // 4 == iota((32, groups), 1))
    tall = matmul(repeat, grid.astype(BF16))
    keep = iota((32, LANES), 0) % 4 == iota((32, LANES), 1) // 32
    masked = jnp.concatenate(
        [
            jnp.where(keep, tall[:, m * LANES : (m + 1) * LANES], 0.0)
            for m in range(terms + zones)
        ],
        axis=0,
    ).astype(BF16)
    tiled = matmul(masked, fold_matrix())
    diagonal = block_mask()
    tables = tiled[: terms * 32]
    first_only = jnp.where(iota(tables.shape, 1) < 32, tables, 0.0).astype(BF16)
    for z in range(zones):
        m = terms + z
        block = tiled[m * 32 : (m + 1) * 32].astype(BF16)
        product = matmul(first_only, jnp.concatenate([block] * 4, axis=0))
        for p in range(terms):
            piece = product[p * 32 : (p + 1) * 32]
            at = (z * terms + p) * LANES
            chain_ref[at : at + LANES, :] = jnp.where(
                diagonal, jnp.concatenate([piece] * 4, axis=0), 0.0
            ).astype(BF16)
    lane_term = iota((32, LANES), 1) // 32
    side = sum(
        jnp.where(lane_term == q, tables[q * 32 : (q + 1) * 32], 0.0) for q in range(terms)
    ).astype(BF16)
    row = iota((LANES, LANES), 0)
    column = iota((LANES, LANES), 1) % 64
    for low_row in range(4):
        move = ones_where(
            (row % 4 == low_row) & (column == ((row % 32) // 4) * SUBS + row // 32)
        )
        spread_ref[low_row * 32 : (low_row + 1) * 32, :] = matmul(side, move).astype(BF16)


def finish_kernel(
    piece_refs_count,
    *refs,
):
    pieces = refs[:piece_refs_count]
    (slot_ref, own_ref, chain_ref, spread_ref, start_ref, centre_ref, contour_ref, radial_hbm,
     out_ref, flat_ref, radial_ref, sem) = refs[piece_refs_count:]
    copy = pltpu.make_async_copy(radial_hbm, radial_ref, sem)
    copy.start()
    zones = out_ref.shape[0]
    near = jnp.concatenate([ref[...] for ref in pieces], axis=0)
    far = matmul(slot_ref[...], near)
    size = own_ref.shape[0]
    weights = own_ref[...] + far[:size] + far[size:]
    per_zone = size // zones
    terms = per_zone // SUBS
    groups = weights.shape[1] // LANES
    diagonal = block_mask()
    fold = fold_matrix()
    flat_ref[...] = jnp.zeros(flat_ref.shape, F32)
    for z in range(zones):
        base = z * per_zone
        lhs = jnp.concatenate(
            [
                jnp.concatenate(
                    [
                        weights[base + p * SUBS : base + (p + 1) * SUBS, g * LANES : (g + 1) * LANES]
                        for p in range(terms)
                    ],
                    axis=1,
                )
                for g in range(groups)
            ],
            axis=0,
        )
        rows = groups * SUBS
        both = matmul(
            jnp.concatenate(split(lhs), axis=0),
            chain_ref[z * terms * LANES : (z + 1) * terms * LANES, :],
        )
        sums = both[:rows] + both[rows:] + start_ref[z * rows : (z + 1) * rows, :]
        field = matmul(spread_ref[...], jnp.concatenate(split(sums), axis=0))
        field = jnp.where(diagonal, field, 0.0)
        field = field[0:32] + field[32:64] + field[64:96] + field[96:128]
        both = matmul(jnp.concatenate(split(field), axis=0), fold)
        field = (both[:32] + both[32:]).astype(BF16).astype(F32)
        block = jnp.where(diagonal, jnp.concatenate([field] * 4, axis=0), 0.0).astype(BF16)
        centre = centre_ref[z * groups : (z + 1) * groups, :]
        central = centre + matmul(centre.astype(BF16), block)
        for g in range(groups):
            flat_ref[z : z + 1, g * LANES : (g + 1) * LANES] = central[g : g + 1]
    central = flat_ref[...].astype(BF16)
    copy.wait()
    out_ref[...] = contour_ref[0] * matmul(central, radial_ref[...])[:zones]


def vmem():
    return pl.BlockSpec(memory_space=pltpu.VMEM)


def smem():
    return pl.BlockSpec(memory_space=pltpu.SMEM)


def sum_over(value, axis):
    size = lax.axis_size(axis)
    if size & (size - 1):
        return lax.psum(value, axis)
    stride = 1
    while stride < size:
        radix = min(4, size // stride)
        parts = [value] + [
            lax.ppermute(value, axis, [(i, i ^ (stride * k)) for i in range(size)])
            for k in range(1, radix)
        ]
        value = (parts[0] + parts[1]) + (parts[2] + parts[3]) if radix == 4 else parts[0] + parts[1]
        stride *= radix
    return value


def shards(
    single_site, coupling, angular, phases, contour, radial, neighbours, owner_row, old_potential
):
    site = single_site[0]
    owned, width = site.shape
    count, zones, places = neighbours.shape
    terms = angular.shape[0]
    atoms = owner_row.shape[0]
    assert owned <= 256 and count <= 256 and places <= LANES and zones == 2
    assert width == 1024 and terms == 4 and atoms % LANES == 0
    table = owner_row.reshape(atoms // LANES, LANES)
    packs = pl.pallas_call(
        functools.partial(pack_kernel, "dom"),
        out_shape=[jax.ShapeDtypeStruct((CAP, width), BF16)] * len(OFFSETS),
        in_specs=[vmem()] * 3,
        out_specs=[vmem()] * len(OFFSETS),
        scratch_shapes=[pltpu.VMEM((len(OFFSETS) * zones, LANES), jnp.int32)],
        name="pack",
    )(neighbours, table, site)
    pieces = [
        lax.ppermute(pack, "dom", [((i - offset) % count, i) for i in range(count)])
        for pack, offset in zip(packs, OFFSETS)
    ]
    first = coupling[:, :, :places]
    last = coupling.reshape(zones, terms, places, places)[:, :, :, 0]
    size = zones * terms * SUBS
    groups = width // LANES
    prepared = pl.pallas_call(
        functools.partial(prepare_kernel, "dom"),
        out_shape=[
            jax.ShapeDtypeStruct((2 * size, CAP * len(OFFSETS)), BF16),
            jax.ShapeDtypeStruct((size, width), F32),
            jax.ShapeDtypeStruct((zones * terms * LANES, LANES), BF16),
            jax.ShapeDtypeStruct((LANES, LANES), BF16),
            jax.ShapeDtypeStruct((zones * groups * SUBS, LANES), F32),
            jax.ShapeDtypeStruct((zones * groups, LANES), F32),
        ],
        in_specs=[vmem()] * 5 + [smem(), vmem()],
        out_specs=[vmem()] * 6,
        scratch_shapes=[
            pltpu.VMEM((zones, LANES), jnp.int32),
            pltpu.VMEM((2 * zones * SUBS, LANES), F32),
            pltpu.VMEM((groups, (terms + zones) * LANES), F32),
        ],
        name="prepare",
    )(neighbours, table, site, first, last, phases, angular)
    part = pl.pallas_call(
        functools.partial(finish_kernel, len(pieces)),
        out_shape=jax.ShapeDtypeStruct((zones, radial.shape[2]), F32),
        in_specs=[vmem()] * (len(pieces) + 6) + [smem(), pl.BlockSpec(memory_space=pltpu.HBM)],
        out_specs=vmem(),
        scratch_shapes=[
            pltpu.VMEM((SUBS, width), F32),
            pltpu.VMEM(radial.shape[1:], BF16),
            pltpu.SemaphoreType.DMA,
        ],
        name="finish",
    )(*pieces, *prepared, contour, radial[0])
    density = sum_over(part, "en")
    return 0.5 * old_potential + 0.5 * density * lax.rsqrt(1.0 + density * density)


def solution(mesh):
    return jax.shard_map(
        shards,
        mesh=mesh,
        in_specs=(
            P("en", "dom", None),
            P("dom", None, None),
            P(),
            P("en", None),
            P("en"),
            P("en", None, None),
            P(),
            P(),
            P("dom", None),
        ),
        out_specs=P("dom", None),
        check_vma=False,
    )
```

```python
import functools

import jax
import jax.numpy as jnp
from jax import lax
from jax.experimental import pallas as pl
from jax.experimental.pallas import tpu as pltpu
from jax.sharding import PartitionSpec as P

REACH = 2
CAP = 48
LIMIT = 24 << 20
LANES = 128
SUBS = 8
OFFSETS = tuple(offset for offset in range(-REACH, REACH + 1) if offset != 0)
F32 = jnp.float32
BF16 = jnp.bfloat16


def matmul(a, b, dims=((1,), (0,))):
    return lax.dot_general(a, b, (dims, ((), ())), preferred_element_type=F32)


def iota(shape, axis):
    return lax.broadcasted_iota(jnp.int32, shape, axis)


def ones_where(mask):
    return jnp.where(mask, 1.0, 0.0).astype(BF16)


def split(x):
    high = x.astype(BF16)
    return high, (x - high.astype(F32)).astype(BF16)


def load_lists(nbr_ref, pad_ref, targets):
    zones, places = nbr_ref.shape[1:]
    pad_ref[...] = jnp.full(pad_ref.shape, -1, jnp.int32)
    for k, target in enumerate(targets):
        pad_ref[k * zones : (k + 1) * zones, 0:places] = nbr_ref[target]
    return jnp.concatenate(
        [pad_ref[r : r + 1, :] for r in range(len(targets) * zones)], axis=1
    )


def resolve(atoms, table_ref, owned):
    table = table_ref[...]
    if owned & (owned - 1) == 0:
        shift = owned.bit_length() - 1
        domain, local = table >> shift, table & (owned - 1)
    else:
        domain, local = table // owned, table % owned
    both = jnp.concatenate([domain, local], axis=1).astype(F32).astype(BF16)
    width = atoms.shape[1]
    row_hot = ones_where(iota((table.shape[0], width), 0) == (atoms >> 7))
    picked = matmul(both, row_hot, ((0,), (0,)))
    lane_hot = iota((LANES, width), 0) == (atoms & (LANES - 1))
    found = [
        jnp.sum(jnp.where(lane_hot, picked[i * LANES : (i + 1) * LANES], 0.0), axis=0, keepdims=True)
        for i in range(2)
    ]
    return jnp.where(atoms < 0, -1.0, found[0]), found[1]


def slot_hot(masks):
    width = masks[0].shape[1]
    rows = jnp.concatenate(
        [jnp.where(mask, 1.0, 0.0) for mask in masks]
        + [jnp.zeros((SUBS - len(masks), width), F32)],
        axis=0,
    ).astype(BF16)
    earlier = ones_where(iota((width, width), 0) < iota((width, width), 1))
    rank = matmul(rows, earlier)
    slots = iota((CAP, width), 0).astype(F32)
    return [
        ones_where((rank[k : k + 1] == slots) & mask) for k, mask in enumerate(masks)
    ]


def pack_kernel(axis, inputs, *refs):
    sources, refs = refs[:inputs], refs[inputs:]
    kept, refs = refs[:inputs], refs[inputs:]
    pack_refs, (pad_ref, sems) = refs[:-2], refs[-2:]
    copies = [
        pltpu.make_async_copy(source, ref, sems.at[k])
        for k, (source, ref) in enumerate(zip(sources, kept))
    ]
    for copy in copies:
        copy.start()
    nbr_ref, table_ref, site_ref = kept[:3]
    count = nbr_ref.shape[0]
    owned = site_ref.shape[0]
    me = lax.axis_index(axis)
    copies[0].wait()
    copies[1].wait()
    atoms = load_lists(nbr_ref, pad_ref, [lax.rem(me + o + count, count) for o in OFFSETS])
    domain, local = resolve(atoms, table_ref, owned)
    width = atoms.shape[1] // len(OFFSETS)
    mine = domain == me.astype(F32)
    spans = [slice(k * width, (k + 1) * width) for k in range(len(OFFSETS))]
    hots = slot_hot([mine[:, s] for s in spans])
    rows = iota((owned, width), 0).astype(F32)
    chosen = [
        matmul(hot, ones_where(local[:, s] == rows), ((1,), (1,))).astype(BF16)
        for hot, s in zip(hots, spans)
    ]
    for copy in copies[2:]:
        copy.wait()
    packed = matmul(jnp.concatenate(chosen, axis=0), site_ref[...]).astype(BF16)
    for k, pack_ref in enumerate(pack_refs):
        pack_ref[...] = packed[k * CAP : (k + 1) * CAP]


def fold_matrix():
    return ones_where(
        (iota((LANES, LANES), 0) % 32) == (iota((LANES, LANES), 1) % 32)
    )


def block_mask():
    return (iota((LANES, LANES), 0) // 32) == (iota((LANES, LANES), 1) // 32)


def strided_row(couple_ref, zone, places):
    terms, width = couple_ref.shape[1:]
    lane = iota((terms, LANES), 1)
    merged = jnp.zeros((terms, LANES), F32)
    for begin in range(0, width, LANES):
        size = min(LANES, width - begin)
        block = couple_ref[zone, :, begin : begin + size].astype(F32)
        if size < LANES:
            spare = jnp.zeros((terms, LANES - size), F32)
            block = jnp.concatenate([block, spare], axis=1)
        kept = functools.reduce(
            jnp.logical_or,
            [lane == at - begin for at in range(0, width, places) if begin <= at < begin + size],
            lane < 0,
        )
        merged = jnp.where(kept, block, merged)
    order = ones_where(
        (iota((LANES, LANES), 1) * places) % LANES == iota((LANES, LANES), 0)
    )
    return matmul(merged.astype(BF16), order)


def prepare_kernel(
    axis,
    nbr_ref, table_ref, site_ref, couple_ref, angular_ref, phase_ref, radial_hbm,
    slot_ref, own_ref, chain_ref, spread_ref, start_ref, centre_ref, radial_ref,
    pad_ref, scaled_ref, grid_ref, sem,
):
    fetch = pltpu.make_async_copy(radial_hbm, radial_ref, sem)
    fetch.start()
    count, zones, places = nbr_ref.shape
    owned = site_ref.shape[0]
    terms = angular_ref.shape[0]
    groups = angular_ref.shape[1] // LANES
    me = lax.axis_index(axis)
    atoms = load_lists(nbr_ref, pad_ref, [me])
    domain, local = resolve(atoms, table_ref, owned)
    width = atoms.shape[1]
    hots = slot_hot(
        [domain == lax.rem(me - o + count, count).astype(F32) for o in OFFSETS]
    )
    scaled_ref[...] = jnp.zeros(scaled_ref.shape, F32)
    lasts = [strided_row(couple_ref, z, places) for z in range(zones)]
    for z in range(zones):
        for q in range(terms):
            phase = phase_ref[0, q]
            for half, rows in enumerate((couple_ref[z, :, 0:places].astype(F32), lasts[z])):
                row = (phase * rows[q : q + 1, 0:places]).astype(BF16)
                at = half * zones * SUBS + z * SUBS + q
                scaled_ref[at : at + 1, 0:places] = row.astype(F32)
    coefs = []
    for z in range(zones):
        to_first = scaled_ref[z * SUBS : (z + 1) * SUBS, :]
        at = (zones + z) * SUBS
        rows = jnp.concatenate(
            [scaled_ref[at + p : at + p + 1, :] * to_first for p in range(terms)], axis=0
        )
        blank = jnp.zeros(rows.shape, F32)
        coefs.append(
            jnp.concatenate([rows if y == z else blank for y in range(zones)], axis=1)
        )
    high, low = split(jnp.concatenate(coefs, axis=0))
    size = high.shape[0]
    both = jnp.concatenate([high, low], axis=0)
    slot_ref[...] = matmul(both, jnp.concatenate(hots, axis=0), ((1,), (1,))).astype(BF16)
    centres = ones_where(
        iota((2 * SUBS, width), 1) == iota((2 * SUBS, width), 0) * LANES
    )
    own_hot = ones_where(
        (local == iota((owned, width), 0).astype(F32)) & (domain == me.astype(F32))
    )
    own_coefs = matmul(jnp.concatenate([both, centres], axis=0), own_hot, ((1,), (1,)))
    own = matmul(own_coefs.astype(BF16), site_ref[...])
    own_ref[...] = own[:size] + own[size : 2 * size]
    centre = own[2 * size : 2 * size + zones]

    for g in range(groups):
        at = slice(g * LANES, (g + 1) * LANES)
        for q in range(terms):
            grid_ref[g : g + 1, q * LANES : (q + 1) * LANES] = angular_ref[q : q + 1, at].astype(F32)
        for z in range(zones):
            m = terms + z
            grid_ref[g : g + 1, m * LANES : (m + 1) * LANES] = centre[z : z + 1, at]
    grid = grid_ref[...]
    for z in range(zones):
        m = terms + z
        centre_ref[z * groups : (z + 1) * groups, :] = grid[:, m * LANES : (m + 1) * LANES]
        start_ref[z * groups * SUBS : (z + 1) * groups * SUBS, :] = jnp.concatenate(
            [
                scaled_ref[z * SUBS : (z + 1) * SUBS, 0:1] * grid[g : g + 1, m * LANES : (m + 1) * LANES]
                for g in range(groups)
            ],
            axis=0,
        )
    repeat = ones_where(iota((32, groups), 0) // 4 == iota((32, groups), 1))
    tall = matmul(repeat, grid.astype(BF16))
    keep = iota((32, LANES), 0) % 4 == iota((32, LANES), 1) // 32
    masked = jnp.concatenate(
        [
            jnp.where(keep, tall[:, m * LANES : (m + 1) * LANES], 0.0)
            for m in range(terms + zones)
        ],
        axis=0,
    ).astype(BF16)
    tiled = matmul(masked, fold_matrix())
    diagonal = block_mask()
    tables = tiled[: terms * 32]
    first_only = jnp.where(iota(tables.shape, 1) < 32, tables, 0.0).astype(BF16)
    for z in range(zones):
        m = terms + z
        block = tiled[m * 32 : (m + 1) * 32].astype(BF16)
        product = matmul(first_only, jnp.concatenate([block] * 4, axis=0))
        for p in range(terms):
            piece = product[p * 32 : (p + 1) * 32]
            at = (z * terms + p) * LANES
            chain_ref[at : at + LANES, :] = jnp.where(
                diagonal, jnp.concatenate([piece] * 4, axis=0), 0.0
            ).astype(BF16)
    lane_term = iota((32, LANES), 1) // 32
    side = sum(
        jnp.where(lane_term == q, tables[q * 32 : (q + 1) * 32], 0.0) for q in range(terms)
    ).astype(BF16)
    row = iota((LANES, LANES), 0)
    column = iota((LANES, LANES), 1) % 64
    for low_row in range(4):
        move = ones_where(
            (row % 4 == low_row) & (column == ((row % 32) // 4) * SUBS + row // 32)
        )
        spread_ref[low_row * 32 : (low_row + 1) * 32, :] = matmul(side, move).astype(BF16)
    fetch.wait()


def finish_kernel(
    piece_refs_count,
    *refs,
):
    pieces = refs[:piece_refs_count]
    (slot_ref, own_ref, chain_ref, spread_ref, start_ref, centre_ref, radial_ref, contour_ref,
     out_ref, flat_ref) = refs[piece_refs_count:]
    zones = out_ref.shape[0]
    near = jnp.concatenate([ref[...] for ref in pieces], axis=0)
    far = matmul(slot_ref[...], near)
    size = own_ref.shape[0]
    weights = own_ref[...] + far[:size] + far[size:]
    per_zone = size // zones
    terms = per_zone // SUBS
    groups = weights.shape[1] // LANES
    diagonal = block_mask()
    fold = fold_matrix()
    flat_ref[...] = jnp.zeros(flat_ref.shape, F32)
    for z in range(zones):
        base = z * per_zone
        lhs = jnp.concatenate(
            [
                jnp.concatenate(
                    [
                        weights[base + p * SUBS : base + (p + 1) * SUBS, g * LANES : (g + 1) * LANES]
                        for p in range(terms)
                    ],
                    axis=1,
                )
                for g in range(groups)
            ],
            axis=0,
        )
        rows = groups * SUBS
        both = matmul(
            jnp.concatenate(split(lhs), axis=0),
            chain_ref[z * terms * LANES : (z + 1) * terms * LANES, :],
        )
        sums = both[:rows] + both[rows:] + start_ref[z * rows : (z + 1) * rows, :]
        field = matmul(spread_ref[...], jnp.concatenate(split(sums), axis=0))
        field = jnp.where(diagonal, field, 0.0)
        field = field[0:32] + field[32:64] + field[64:96] + field[96:128]
        both = matmul(jnp.concatenate(split(field), axis=0), fold)
        field = (both[:32] + both[32:]).astype(BF16).astype(F32)
        block = jnp.where(diagonal, jnp.concatenate([field] * 4, axis=0), 0.0).astype(BF16)
        centre = centre_ref[z * groups : (z + 1) * groups, :]
        central = centre + matmul(centre.astype(BF16), block)
        for g in range(groups):
            flat_ref[z : z + 1, g * LANES : (g + 1) * LANES] = central[g : g + 1]
    central = flat_ref[...].astype(BF16)
    out_ref[...] = contour_ref[0] * matmul(central, radial_ref[...], ((1,), (1,)))[:zones]


def vmem():
    return pl.BlockSpec(memory_space=pltpu.VMEM)


def smem():
    return pl.BlockSpec(memory_space=pltpu.SMEM)


def sum_over(value, axis):
    size = lax.axis_size(axis)
    if size & (size - 1):
        return lax.psum(value, axis)
    stride = 1
    while stride < size:
        radix = min(4, size // stride)
        parts = [value] + [
            lax.ppermute(value, axis, [(i, i ^ (stride * k)) for i in range(size)])
            for k in range(1, radix)
        ]
        value = (parts[0] + parts[1]) + (parts[2] + parts[3]) if radix == 4 else parts[0] + parts[1]
        stride *= radix
    return value


def shards(
    single_site, coupling, angular, phases, contour, radial, neighbours, owner_row, old_potential
):
    site = single_site[0]
    owned, width = site.shape
    count, zones, places = neighbours.shape
    terms = angular.shape[0]
    atoms = owner_row.shape[0]
    assert owned <= 256 and count <= 256 and places <= LANES and zones == 2
    assert width == 1024 and terms == 4 and atoms % LANES == 0 and places % 2 == 1
    table = owner_row.reshape(atoms // LANES, LANES)
    sources = [neighbours, table, site, coupling, angular]
    results = pl.pallas_call(
        functools.partial(pack_kernel, "dom", len(sources)),
        out_shape=[pltpu.VMEM(x.shape, x.dtype) for x in sources]
        + [pltpu.VMEM((CAP, width), BF16)] * len(OFFSETS),
        in_specs=[pl.BlockSpec(memory_space=pltpu.HBM)] * len(sources),
        out_specs=[vmem()] * (len(sources) + len(OFFSETS)),
        scratch_shapes=[
            pltpu.VMEM((len(OFFSETS) * zones, LANES), jnp.int32),
            pltpu.SemaphoreType.DMA((len(sources),)),
        ],
        compiler_params=pltpu.CompilerParams(vmem_limit_bytes=LIMIT),
        name="pack",
    )(*[pltpu.with_memory_space_constraint(x, pltpu.HBM) for x in sources])
    kept, packs = results[: len(sources)], results[len(sources) :]
    pieces = [
        lax.ppermute(pack, "dom", [((i - offset) % count, i) for i in range(count)])
        for pack, offset in zip(packs, OFFSETS)
    ]
    size = zones * terms * SUBS
    groups = width // LANES
    prepared = pl.pallas_call(
        functools.partial(prepare_kernel, "dom"),
        out_shape=[
            pltpu.VMEM((2 * size, CAP * len(OFFSETS)), BF16),
            pltpu.VMEM((size, width), F32),
            pltpu.VMEM((zones * terms * LANES, LANES), BF16),
            pltpu.VMEM((LANES, LANES), BF16),
            pltpu.VMEM((zones * groups * SUBS, LANES), F32),
            pltpu.VMEM((zones * groups, LANES), F32),
            pltpu.VMEM((radial.shape[2], width), BF16),
        ],
        in_specs=[vmem()] * 5 + [smem(), pl.BlockSpec(memory_space=pltpu.HBM)],
        out_specs=[vmem()] * 7,
        scratch_shapes=[
            pltpu.VMEM((zones, LANES), jnp.int32),
            pltpu.VMEM((2 * zones * SUBS, LANES), F32),
            pltpu.VMEM((groups, (terms + zones) * LANES), F32),
            pltpu.SemaphoreType.DMA,
        ],
        compiler_params=pltpu.CompilerParams(vmem_limit_bytes=LIMIT),
        name="prepare",
    )(*kept, phases, pltpu.with_memory_space_constraint(radial[0].T, pltpu.HBM))
    pieces = [pltpu.with_memory_space_constraint(piece, pltpu.VMEM) for piece in pieces]
    part = pl.pallas_call(
        functools.partial(finish_kernel, len(pieces)),
        out_shape=pltpu.VMEM((zones, radial.shape[2]), F32),
        in_specs=[vmem()] * (len(pieces) + 7) + [smem()],
        out_specs=vmem(),
        scratch_shapes=[pltpu.VMEM((SUBS, width), F32)],
        compiler_params=pltpu.CompilerParams(vmem_limit_bytes=LIMIT),
        name="finish",
    )(*pieces, *prepared, contour)
    density = sum_over(part, "en")
    return 0.5 * old_potential + 0.5 * density * lax.rsqrt(1.0 + density * density)


def solution(mesh):
    return jax.shard_map(
        shards,
        mesh=mesh,
        in_specs=(
            P("en", "dom", None),
            P("dom", None, None),
            P(),
            P("en", None),
            P("en"),
            P("en", None, None),
            P(),
            P(),
            P("dom", None),
        ),
        out_specs=P("dom", None),
        check_vma=False,
    )
```

```python
import functools

import jax
import jax.numpy as jnp
from jax import lax
from jax.experimental import pallas as pl
from jax.experimental.pallas import tpu as pltpu
from jax.sharding import PartitionSpec as P


REACH = 2
CAP = 48
LIMIT = 24 << 20
LANES = 128
SUBS = 8
SHIFTS = (1, 2, -2, -1)
PARTS = (4,19)
F32 = jnp.float32
BF16 = jnp.bfloat16


def matmul(a, b, dims=((1,), (0,))):
    return lax.dot_general(a, b, (dims, ((), ())), preferred_element_type=F32)


def iota(shape, axis):
    return lax.broadcasted_iota(jnp.int32, shape, axis)


def ones_where(mask):
    return jnp.where(mask, 1.0, 0.0).astype(BF16)


def split(x):
    high = x.astype(BF16)
    return high, (x - high.astype(F32)).astype(BF16)


def load_lists(nbr_ref, pad_ref, targets):
    zones, places = nbr_ref.shape[1:]
    pad_ref[...] = jnp.full(pad_ref.shape, -1, jnp.int32)
    for k, target in enumerate(targets):
        pad_ref[k * zones : (k + 1) * zones, 0:places] = nbr_ref[target]
    return jnp.concatenate(
        [pad_ref[r : r + 1, :] for r in range(len(targets) * zones)], axis=1
    )


def resolve(atoms, table_ref, owned):
    table = table_ref[...]
    if owned & (owned - 1) == 0:
        shift = owned.bit_length() - 1
        domain, local = table >> shift, table & (owned - 1)
    else:
        domain, local = table // owned, table % owned
    both = jnp.concatenate([domain, local], axis=1).astype(F32).astype(BF16)
    width = atoms.shape[1]
    row_hot = ones_where(iota((table.shape[0], width), 0) == (atoms >> 7))
    picked = matmul(both, row_hot, ((0,), (0,)))
    lane_hot = iota((LANES, width), 0) == (atoms & (LANES - 1))
    found = [
        jnp.sum(jnp.where(lane_hot, picked[i * LANES : (i + 1) * LANES], 0.0), axis=0, keepdims=True)
        for i in range(2)
    ]
    return jnp.where(atoms < 0, -1.0, found[0]), found[1]


def slot_hot(masks):
    width = masks[0].shape[1]
    rows = jnp.concatenate(
        [jnp.where(mask, 1.0, 0.0) for mask in masks]
        + [jnp.zeros((SUBS - len(masks), width), F32)],
        axis=0,
    ).astype(BF16)
    earlier = ones_where(iota((width, width), 0) < iota((width, width), 1))
    rank = matmul(rows, earlier)
    slots = iota((CAP, width), 0).astype(F32)
    return [
        ones_where((rank[k : k + 1] == slots) & mask) for k, mask in enumerate(masks)
    ]


def pack_kernel(axis, inputs, *refs):
    sources, radial_hbm, refs = refs[:inputs], refs[inputs], refs[inputs + 1 :]
    kept, radial_ref, refs = refs[:inputs], refs[inputs], refs[inputs + 1 :]
    pack_refs, (pad_ref, sems) = refs[:-2], refs[-2:]
    copies = [
        pltpu.make_async_copy(source, ref, sems.at[k])
        for k, (source, ref) in enumerate(zip(sources, kept))
    ]
    copies.append(
        pltpu.make_async_copy(
            radial_hbm.at[0 : radial_ref.shape[0]], radial_ref, sems.at[inputs]
        )
    )
    for copy in copies:
        copy.start()
    nbr_ref, table_ref, site_ref = kept[:3]
    count = nbr_ref.shape[0]
    owned = site_ref.shape[0]
    me = lax.axis_index(axis)
    copies[0].wait()
    copies[1].wait()
    atoms = load_lists(nbr_ref, pad_ref, [lax.rem(me + shift + count, count) for shift in SHIFTS])
    domain, local = resolve(atoms, table_ref, owned)
    width = atoms.shape[1] // len(SHIFTS)
    mine = domain == me.astype(F32)
    spans = [slice(k * width, (k + 1) * width) for k in range(len(SHIFTS))]
    hots = slot_hot([mine[:, s] for s in spans])
    rows = iota((owned, width), 0).astype(F32)
    chosen = [
        matmul(hot, ones_where(local[:, s] == rows), ((1,), (1,))).astype(BF16)
        for hot, s in zip(hots, spans)
    ]
    for copy in copies[2:-1]:
        copy.wait()
    packed = matmul(jnp.concatenate(chosen, axis=0), site_ref[...]).astype(BF16)
    for k, pack_ref in enumerate(pack_refs):
        pack_ref[...] = packed[k * CAP : (k + 1) * CAP]
    copies[-1].wait()


def fold_matrix():
    return ones_where(
        (iota((LANES, LANES), 0) % 32) == (iota((LANES, LANES), 1) % 32)
    )


def block_mask():
    return (iota((LANES, LANES), 0) // 32) == (iota((LANES, LANES), 1) // 32)


def strided_row(couple_ref, zone, places):
    terms, width = couple_ref.shape[1:]
    lane = iota((terms, LANES), 1)
    merged = jnp.zeros((terms, LANES), F32)
    for begin in range(0, width, LANES):
        size = min(LANES, width - begin)
        block = couple_ref[zone, :, begin : begin + size].astype(F32)
        if size < LANES:
            spare = jnp.zeros((terms, LANES - size), F32)
            block = jnp.concatenate([block, spare], axis=1)
        kept = functools.reduce(
            jnp.logical_or,
            [lane == at - begin for at in range(0, width, places) if begin <= at < begin + size],
            lane < 0,
        )
        merged = jnp.where(kept, block, merged)
    order = ones_where(
        (iota((LANES, LANES), 1) * places) % LANES == iota((LANES, LANES), 0)
    )
    return matmul(merged.astype(BF16), order)


def prepare_kernel(
    axis, begin,
    nbr_ref, table_ref, site_ref, couple_ref, angular_ref, phase_ref, radial_hbm,
    slot_ref, own_ref, chain_ref, spread_ref, start_ref, centre_ref, radial_ref,
    pad_ref, scaled_ref, grid_ref, sem,
):
    fetch = pltpu.make_async_copy(
        radial_hbm.at[begin : begin + radial_ref.shape[0]], radial_ref, sem
    )
    fetch.start()
    count, zones, places = nbr_ref.shape
    owned = site_ref.shape[0]
    terms = angular_ref.shape[0]
    groups = angular_ref.shape[1] // LANES
    me = lax.axis_index(axis)
    atoms = load_lists(nbr_ref, pad_ref, [me])
    domain, local = resolve(atoms, table_ref, owned)
    width = atoms.shape[1]
    hots = slot_hot(
        [domain == lax.rem(me - shift + count, count).astype(F32) for shift in SHIFTS]
    )
    scaled_ref[...] = jnp.zeros(scaled_ref.shape, F32)
    lasts = [strided_row(couple_ref, z, places) for z in range(zones)]
    for z in range(zones):
        for q in range(terms):
            phase = phase_ref[0:1, q : q + 1]
            for half, rows in enumerate((couple_ref[z, :, 0:places].astype(F32), lasts[z])):
                row = (phase * rows[q : q + 1, 0:places]).astype(BF16)
                at = half * zones * SUBS + z * SUBS + q
                scaled_ref[at : at + 1, 0:places] = row.astype(F32)
    coefs = []
    for z in range(zones):
        to_first = scaled_ref[z * SUBS : (z + 1) * SUBS, :]
        at = (zones + z) * SUBS
        rows = jnp.concatenate(
            [scaled_ref[at + p : at + p + 1, :] * to_first for p in range(terms)], axis=0
        )
        blank = jnp.zeros(rows.shape, F32)
        coefs.append(
            jnp.concatenate([rows if y == z else blank for y in range(zones)], axis=1)
        )
    high, low = split(jnp.concatenate(coefs, axis=0))
    size = high.shape[0]
    both = jnp.concatenate([high, low], axis=0)
    slot_ref[...] = matmul(both, jnp.concatenate(hots, axis=0), ((1,), (1,))).astype(BF16)
    centres = ones_where(
        iota((2 * SUBS, width), 1) == iota((2 * SUBS, width), 0) * LANES
    )
    own_hot = ones_where(
        (local == iota((owned, width), 0).astype(F32)) & (domain == me.astype(F32))
    )
    own_coefs = matmul(jnp.concatenate([both, centres], axis=0), own_hot, ((1,), (1,)))
    own = matmul(own_coefs.astype(BF16), site_ref[...])
    own_ref[...] = own[:size] + own[size : 2 * size]
    centre = own[2 * size : 2 * size + zones]

    for g in range(groups):
        at = slice(g * LANES, (g + 1) * LANES)
        for q in range(terms):
            grid_ref[g : g + 1, q * LANES : (q + 1) * LANES] = angular_ref[q : q + 1, at].astype(F32)
        for z in range(zones):
            m = terms + z
            grid_ref[g : g + 1, m * LANES : (m + 1) * LANES] = centre[z : z + 1, at]
    grid = grid_ref[...]
    for z in range(zones):
        m = terms + z
        centre_ref[z * groups : (z + 1) * groups, :] = grid[:, m * LANES : (m + 1) * LANES]
        start_ref[z * groups * SUBS : (z + 1) * groups * SUBS, :] = jnp.concatenate(
            [
                scaled_ref[z * SUBS : (z + 1) * SUBS, 0:1] * grid[g : g + 1, m * LANES : (m + 1) * LANES]
                for g in range(groups)
            ],
            axis=0,
        )
    repeat = ones_where(iota((32, groups), 0) // 4 == iota((32, groups), 1))
    tall = matmul(repeat, grid.astype(BF16))
    keep = iota((32, LANES), 0) % 4 == iota((32, LANES), 1) // 32
    masked = jnp.concatenate(
        [
            jnp.where(keep, tall[:, m * LANES : (m + 1) * LANES], 0.0)
            for m in range(terms + zones)
        ],
        axis=0,
    ).astype(BF16)
    tiled = matmul(masked, fold_matrix())
    diagonal = block_mask()
    tables = tiled[: terms * 32]
    first_only = jnp.where(iota(tables.shape, 1) < 32, tables, 0.0).astype(BF16)
    for z in range(zones):
        m = terms + z
        block = tiled[m * 32 : (m + 1) * 32].astype(BF16)
        product = matmul(first_only, jnp.concatenate([block] * 4, axis=0))
        for p in range(terms):
            piece = product[p * 32 : (p + 1) * 32]
            at = (z * terms + p) * LANES
            chain_ref[at : at + LANES, :] = jnp.where(
                diagonal, jnp.concatenate([piece] * 4, axis=0), 0.0
            ).astype(BF16)
    lane_term = iota((32, LANES), 1) // 32
    side = sum(
        jnp.where(lane_term == q, tables[q * 32 : (q + 1) * 32], 0.0) for q in range(terms)
    ).astype(BF16)
    row = iota((LANES, 2 * LANES), 0)
    column = iota((LANES, 2 * LANES), 1)
    same = (column % SUBS == row // 32) & ((column % 64) // SUBS == (row % 32) // 4)
    for block in range(4):
        move = ones_where(same & (row % 4 == (column // 64 + block) % 4))
        spread_ref[block * 32 : (block + 1) * 32, :] = matmul(side, move).astype(BF16)
    fetch.wait()


def finish_kernel(count, *refs):
    pieces, refs = refs[:count], refs[count:]
    slot_ref, own_ref, chain_ref, spread_ref, start_ref, centre_ref, refs = *refs[:6], refs[6:]
    radial_refs, (contour_ref, radial_hbm, out_ref, flat_ref, tail_ref, sem) = refs[:-6], refs[-6:]
    begin = radial_hbm.shape[0] - tail_ref.shape[0]
    fetch = pltpu.make_async_copy(radial_hbm.at[begin : radial_hbm.shape[0]], tail_ref, sem)
    fetch.start()
    zones = out_ref.shape[0]
    near = jnp.concatenate([ref[...] for ref in pieces], axis=0)
    far = matmul(slot_ref[...], near)
    size = own_ref.shape[0]
    weights = own_ref[...] + far[:size] + far[size:]
    per_zone = size // zones
    terms = per_zone // SUBS
    groups = weights.shape[1] // LANES
    rows = groups * SUBS
    turned = []
    for z in range(zones):
        base = z * per_zone
        lhs = jnp.concatenate(
            [
                jnp.concatenate(
                    [
                        weights[base + p * SUBS : base + (p + 1) * SUBS, g * LANES : (g + 1) * LANES]
                        for p in range(terms)
                    ],
                    axis=1,
                )
                for g in range(groups)
            ],
            axis=0,
        )
        both = matmul(
            jnp.concatenate(split(lhs), axis=0),
            chain_ref[z * terms * LANES : (z + 1) * terms * LANES, :],
        )
        sums = both[:rows] + both[rows:] + start_ref[z * rows : (z + 1) * rows, :]
        turned.append(
            jnp.concatenate(
                [sums] + [pltpu.roll(sums, LANES - 32 * k, 1) for k in range(1, 4)], axis=0
            )
        )
    high, low = split(jnp.concatenate(turned, axis=1))
    spread = spread_ref[...]
    field = matmul(spread, high) + matmul(spread, low)
    diagonal = jnp.concatenate([block_mask()] * zones, axis=1)
    field = jnp.where(diagonal, field, 0.0).astype(BF16)
    centre = centre_ref[...]
    change = matmul(centre.astype(BF16), field)
    flat_ref[...] = jnp.zeros(flat_ref.shape, F32)
    for z in range(zones):
        span = slice(z * groups, (z + 1) * groups)
        central = centre[span] + change[span, z * LANES : (z + 1) * LANES]
        for g in range(groups):
            flat_ref[z : z + 1, g * LANES : (g + 1) * LANES] = central[g : g + 1]
    central = flat_ref[...].astype(BF16)
    scale = contour_ref[0]
    at = 0
    for ref in (*radial_refs, tail_ref):
        if ref is tail_ref:
            fetch.wait()
        part = scale * matmul(central, ref[...], ((1,), (1,)))
        out_ref[:, at : at + ref.shape[0]] = part[:zones].astype(BF16)
        at += ref.shape[0]


def vmem():
    return pl.BlockSpec(memory_space=pltpu.VMEM)


def sum_over(value, axis):
    size = lax.axis_size(axis)
    if size & (size - 1):
        return lax.psum(value.astype(F32), axis)
    stride = 1
    while stride < size:
        value = value.astype(BF16)
        radix = min(4, size // stride)
        parts = {0: value}
        for k in (3, 2, 1):
            if k < radix:
                parts[k] = lax.ppermute(value, axis, [(i, i ^ (stride * k)) for i in range(size)])
        parts = [parts[k].astype(F32) for k in range(radix)]
        value = (parts[0] + parts[1]) + (parts[2] + parts[3]) if radix == 4 else parts[0] + parts[1]
        stride *= radix
    return value


def shards(
    single_site, coupling, angular, phases, contour, radial, neighbours, owner_row, old_potential
):
    site = single_site[0]
    owned, width = site.shape
    count, zones, places = neighbours.shape
    terms = angular.shape[0]
    atoms = owner_row.shape[0]
    assert owned <= 256 and count <= 256 and places <= LANES and zones == 2
    assert count > 2 * REACH and sorted(SHIFTS) == [k for k in range(-REACH, REACH + 1) if k]
    assert width == 1024 and terms == 4 and atoms % LANES == 0 and places % 2 == 1
    table = owner_row.reshape(atoms // LANES, LANES)
    sources = [neighbours, table, site, coupling, angular, phases]
    hbm = pl.BlockSpec(memory_space=pltpu.HBM)
    params = pltpu.CompilerParams(vmem_limit_bytes=LIMIT)
    turned = pltpu.with_memory_space_constraint(radial[0].T, pltpu.HBM)
    parts = [PARTS[0] * LANES, PARTS[1] * LANES]
    results = pl.pallas_call(
        functools.partial(pack_kernel, "dom", len(sources)),
        out_shape=[pltpu.VMEM(x.shape, x.dtype) for x in sources]
        + [pltpu.VMEM((parts[0], width), BF16)]
        + [pltpu.VMEM((CAP, width), BF16)] * len(SHIFTS),
        in_specs=[hbm] * (len(sources) + 1),
        out_specs=[vmem()] * (len(sources) + 1 + len(SHIFTS)),
        scratch_shapes=[
            pltpu.VMEM((len(SHIFTS) * zones, LANES), jnp.int32),
            pltpu.SemaphoreType.DMA((len(sources) + 1,)),
        ],
        compiler_params=params,
        name="pack",
    )(*[pltpu.with_memory_space_constraint(x, pltpu.HBM) for x in sources], turned)
    kept, head, packs = results[: len(sources)], results[len(sources)], results[len(sources) + 1 :]
    pieces = [
        lax.ppermute(pack, "dom", [(i, (i + shift) % count) for i in range(count)])
        for pack, shift in zip(packs, SHIFTS)
    ]
    size = zones * terms * SUBS
    groups = width // LANES
    prepared = pl.pallas_call(
        functools.partial(prepare_kernel, "dom", parts[0]),
        out_shape=[
            pltpu.VMEM((2 * size, CAP * len(SHIFTS)), BF16),
            pltpu.VMEM((size, width), F32),
            pltpu.VMEM((zones * terms * LANES, LANES), BF16),
            pltpu.VMEM((LANES, 2 * LANES), BF16),
            pltpu.VMEM((zones * groups * SUBS, LANES), F32),
            pltpu.VMEM((zones * groups, LANES), F32),
            pltpu.VMEM((parts[1], width), BF16),
        ],
        in_specs=[vmem()] * 6 + [hbm],
        out_specs=[vmem()] * 7,
        scratch_shapes=[
            pltpu.VMEM((zones, LANES), jnp.int32),
            pltpu.VMEM((2 * zones * SUBS, LANES), F32),
            pltpu.VMEM((groups, (terms + zones) * LANES), F32),
            pltpu.SemaphoreType.DMA,
        ],
        compiler_params=params,
        name="prepare",
    )(*kept, turned)
    pieces = [pltpu.with_memory_space_constraint(piece, pltpu.VMEM) for piece in pieces]
    entries = radial.shape[2]
    part = pl.pallas_call(
        functools.partial(finish_kernel, len(pieces)),
        out_shape=pltpu.VMEM((zones, entries), BF16),
        in_specs=[vmem()] * (len(pieces) + 8) + [pl.BlockSpec(memory_space=pltpu.SMEM), hbm],
        out_specs=vmem(),
        scratch_shapes=[
            pltpu.VMEM((SUBS, width), F32),
            pltpu.VMEM((entries - sum(parts), width), BF16),
            pltpu.SemaphoreType.DMA,
        ],
        compiler_params=params,
        name="finish",
    )(*pieces, *prepared[:-1], head, prepared[-1], contour, turned)
    density = sum_over(part, "en")
    return 0.5 * old_potential + 0.5 * density * lax.rsqrt(1.0 + density * density)


def solution(mesh):
    return jax.shard_map(
        shards,
        mesh=mesh,
        in_specs=(
            P("en", "dom", None),
            P("dom", None, None),
            P(),
            P("en", None),
            P("en"),
            P("en", None, None),
            P(),
            P(),
            P("dom", None),
        ),
        out_specs=P("dom", None),
        check_vma=False,
    )
```

```python
import functools

import jax
import jax.numpy as jnp
from jax import lax
from jax.experimental import pallas as pl
from jax.experimental.pallas import tpu as pltpu
from jax.sharding import PartitionSpec as P


REACH = 2
CAP = 48
LIMIT = 24 << 20
LANES = 128
SUBS = 8
SHIFTS = (1, 2, -2, -1)
HEAD = 6
F32 = jnp.float32
BF16 = jnp.bfloat16


def matmul(a, b, dims=((1,), (0,))):
    return lax.dot_general(a, b, (dims, ((), ())), preferred_element_type=F32)


def iota(shape, axis):
    return lax.broadcasted_iota(jnp.int32, shape, axis)


def ones_where(mask):
    return jnp.where(mask, 1.0, 0.0).astype(BF16)


def split(x):
    high = x.astype(BF16)
    return high, (x - high.astype(F32)).astype(BF16)


def load_lists(nbr_ref, pad_ref, targets):
    zones, places = nbr_ref.shape[1:]
    pad_ref[...] = jnp.full(pad_ref.shape, -1, jnp.int32)
    for k, target in enumerate(targets):
        pad_ref[k * zones : (k + 1) * zones, 0:places] = nbr_ref[target]
    return jnp.concatenate(
        [pad_ref[r : r + 1, :] for r in range(len(targets) * zones)], axis=1
    )


def resolve(atoms, table_ref, owned):
    table = table_ref[...]
    height = table.shape[0]
    both = jnp.concatenate([table & ~255, table & 255], axis=0).astype(F32)
    both = jnp.concatenate(
        [both] + [pltpu.roll(both, LANES - 32 * k, 1) for k in range(1, 4)], axis=0
    )[:, :32].astype(BF16)
    width = atoms.shape[1]
    key = ((atoms >> 5) & 3) * height + (atoms >> 7)
    hots = []
    for k in range(4):
        hot = jnp.where(iota((height, width), 0) + k * height == key, 1.0, 0.0)
        hots += [hot, hot]
    picked = matmul(both, jnp.concatenate(hots, axis=0).astype(BF16), ((0,), (0,)))
    lane_hot = iota((32, width), 0) == (atoms & 31)
    found = jnp.sum(jnp.where(lane_hot, picked, 0.0), axis=0, keepdims=True).astype(jnp.int32)
    if owned & (owned - 1) == 0:
        domain, local = found >> (owned.bit_length() - 1), found & (owned - 1)
    else:
        domain, local = found // owned, found % owned
    return jnp.where(atoms < 0, -1, domain), local


def slot_hot(masks):
    width = masks[0].shape[1]
    rows = jnp.concatenate(
        [jnp.where(mask, 1.0, 0.0) for mask in masks]
        + [jnp.zeros((SUBS - len(masks), width), F32)],
        axis=0,
    ).astype(BF16)
    earlier = ones_where(iota((width, width), 0) < iota((width, width), 1))
    rank = matmul(rows, earlier)
    slots = iota((CAP, width), 0).astype(F32)
    return [
        ones_where((rank[k : k + 1] == slots) & mask) for k, mask in enumerate(masks)
    ]


def pack_kernel(axis, inputs, *refs):
    sources, radial_hbm, refs = refs[:inputs], refs[inputs], refs[inputs + 1 :]
    kept, radial_ref, refs = refs[:inputs], refs[inputs], refs[inputs + 1 :]
    pack_refs, (pad_ref, sems) = refs[:-2], refs[-2:]
    copies = [
        pltpu.make_async_copy(source, ref, sems.at[k])
        for k, (source, ref) in enumerate(zip(sources, kept))
    ]
    copies.append(
        pltpu.make_async_copy(
            radial_hbm.at[0 : radial_ref.shape[0]], radial_ref, sems.at[inputs]
        )
    )
    for copy in copies:
        copy.start()
    nbr_ref, table_ref, site_ref = kept[:3]
    count = nbr_ref.shape[0]
    owned = site_ref.shape[0]
    me = lax.axis_index(axis)
    copies[0].wait()
    copies[1].wait()
    atoms = load_lists(nbr_ref, pad_ref, [lax.rem(me + shift + count, count) for shift in SHIFTS])
    domain, local = resolve(atoms, table_ref, owned)
    width = atoms.shape[1] // len(SHIFTS)
    mine = domain == me
    spans = [slice(k * width, (k + 1) * width) for k in range(len(SHIFTS))]
    hots = slot_hot([mine[:, s] for s in spans])
    rows = iota((owned, width), 0)
    chosen = [
        matmul(hot, ones_where(local[:, s] == rows), ((1,), (1,))).astype(BF16)
        for hot, s in zip(hots, spans)
    ]
    for copy in copies[2:-1]:
        copy.wait()
    packed = matmul(jnp.concatenate(chosen, axis=0), site_ref[...]).astype(BF16)
    for k, pack_ref in enumerate(pack_refs):
        pack_ref[...] = packed[k * CAP : (k + 1) * CAP]
    copies[-1].wait()


def fold_matrix():
    return ones_where(
        (iota((LANES, LANES), 0) % 32) == (iota((LANES, LANES), 1) % 32)
    )


def block_mask():
    return (iota((LANES, LANES), 0) // 32) == (iota((LANES, LANES), 1) // 32)


def strided_row(couple_ref, zone, places):
    terms, width = couple_ref.shape[1:]
    lane = iota((terms, LANES), 1)
    merged = jnp.zeros((terms, LANES), F32)
    for begin in range(0, width, LANES):
        size = min(LANES, width - begin)
        block = couple_ref[zone, :, begin : begin + size].astype(F32)
        if size < LANES:
            spare = jnp.zeros((terms, LANES - size), F32)
            block = jnp.concatenate([block, spare], axis=1)
        kept = functools.reduce(
            jnp.logical_or,
            [lane == at - begin for at in range(0, width, places) if begin <= at < begin + size],
            lane < 0,
        )
        merged = jnp.where(kept, block, merged)
    order = ones_where(
        (iota((LANES, LANES), 1) * places) % LANES == iota((LANES, LANES), 0)
    )
    return matmul(merged.astype(BF16), order)


def prepare_kernel(
    axis, begin,
    nbr_ref, table_ref, site_ref, couple_ref, angular_ref, phase_ref, head_ref, radial_hbm,
    slot_ref, own_ref, chain_ref, spread_ref, start_ref, centre_ref, turned_ref, radial_ref,
    pad_ref, scaled_ref, grid_ref, sem,
):
    fetch = pltpu.make_async_copy(
        radial_hbm.at[begin : begin + radial_ref.shape[0]], radial_ref, sem
    )
    fetch.start()
    count, zones, places = nbr_ref.shape
    owned = site_ref.shape[0]
    terms = angular_ref.shape[0]
    groups = angular_ref.shape[1] // LANES
    me = lax.axis_index(axis)
    atoms = load_lists(nbr_ref, pad_ref, [me])
    domain, local = resolve(atoms, table_ref, owned)
    width = atoms.shape[1]
    hots = slot_hot(
        [domain == lax.rem(me - shift + count, count) for shift in SHIFTS]
    )
    scaled_ref[...] = jnp.zeros(scaled_ref.shape, F32)
    lasts = [strided_row(couple_ref, z, places) for z in range(zones)]
    for z in range(zones):
        for q in range(terms):
            phase = phase_ref[0:1, q : q + 1]
            for half, rows in enumerate((couple_ref[z, :, 0:places].astype(F32), lasts[z])):
                row = (phase * rows[q : q + 1, 0:places]).astype(BF16)
                at = half * zones * SUBS + z * SUBS + q
                scaled_ref[at : at + 1, 0:places] = row.astype(F32)
    coefs = []
    for z in range(zones):
        to_first = scaled_ref[z * SUBS : (z + 1) * SUBS, :]
        at = (zones + z) * SUBS
        rows = jnp.concatenate(
            [scaled_ref[at + p : at + p + 1, :] * to_first for p in range(terms)], axis=0
        )
        blank = jnp.zeros(rows.shape, F32)
        coefs.append(
            jnp.concatenate([rows if y == z else blank for y in range(zones)], axis=1)
        )
    high, low = split(jnp.concatenate(coefs, axis=0))
    size = high.shape[0]
    both = jnp.concatenate([high, low], axis=0)
    slot_ref[...] = matmul(both, jnp.concatenate(hots, axis=0), ((1,), (1,))).astype(BF16)
    centres = ones_where(
        iota((2 * SUBS, width), 1) == iota((2 * SUBS, width), 0) * LANES
    )
    own_hot = ones_where(
        (local == iota((owned, width), 0)) & (domain == me)
    )
    own_coefs = matmul(jnp.concatenate([both, centres], axis=0), own_hot, ((1,), (1,)))
    own = matmul(own_coefs.astype(BF16), site_ref[...])
    own_ref[...] = own[:size] + own[size : 2 * size]
    centre = own[2 * size : 2 * size + zones]

    for g in range(groups):
        at = slice(g * LANES, (g + 1) * LANES)
        for q in range(terms):
            grid_ref[g : g + 1, q * LANES : (q + 1) * LANES] = angular_ref[q : q + 1, at].astype(F32)
        for z in range(zones):
            m = terms + z
            grid_ref[g : g + 1, m * LANES : (m + 1) * LANES] = centre[z : z + 1, at]
    grid = grid_ref[...]
    for z in range(zones):
        m = terms + z
        centre_ref[z * groups : (z + 1) * groups, :] = grid[:, m * LANES : (m + 1) * LANES]
        start_ref[z * groups * SUBS : (z + 1) * groups * SUBS, :] = jnp.concatenate(
            [
                scaled_ref[z * SUBS : (z + 1) * SUBS, 0:1] * grid[g : g + 1, m * LANES : (m + 1) * LANES]
                for g in range(groups)
            ],
            axis=0,
        )
    repeat = ones_where(iota((32, groups), 0) // 4 == iota((32, groups), 1))
    tall = matmul(repeat, grid.astype(BF16))
    keep = iota((32, LANES), 0) % 4 == iota((32, LANES), 1) // 32
    masked = jnp.concatenate(
        [
            jnp.where(keep, tall[:, m * LANES : (m + 1) * LANES], 0.0)
            for m in range(terms + zones)
        ],
        axis=0,
    ).astype(BF16)
    tiled = matmul(masked, fold_matrix())
    diagonal = block_mask()
    tables = tiled[: terms * 32]
    first_only = jnp.where(iota(tables.shape, 1) < 32, tables, 0.0).astype(BF16)
    for z in range(zones):
        m = terms + z
        block = tiled[m * 32 : (m + 1) * 32].astype(BF16)
        product = matmul(first_only, jnp.concatenate([block] * 4, axis=0))
        for p in range(terms):
            piece = product[p * 32 : (p + 1) * 32]
            at = (z * terms + p) * LANES
            chain_ref[at : at + LANES, :] = jnp.where(
                diagonal, jnp.concatenate([piece] * 4, axis=0), 0.0
            ).astype(BF16)
    lane_term = iota((32, LANES), 1) // 32
    side = sum(
        jnp.where(lane_term == q, tables[q * 32 : (q + 1) * 32], 0.0) for q in range(terms)
    ).astype(BF16)
    order = ones_where(
        iota((32, 32), 1) == (iota((32, 32), 0) % groups) * 4 + iota((32, 32), 0) // groups
    )
    mixed = []
    for z in range(zones):
        block = tiled[(terms + z) * 32 : (terms + z + 1) * 32].astype(BF16)
        sorted_rows = matmul(order, block).astype(BF16)
        mixed += split(matmul(sorted_rows[:, :32], side))
    row = iota((LANES, 2 * LANES), 0)
    column = iota((LANES, 2 * LANES), 1)
    same = (column % SUBS == row // 32) & ((column % 64) // SUBS == (row % 32) // 4)
    for block in range(4):
        move = ones_where(same & (row % 4 == (column // 64 + block) % 4))
        rows = jnp.concatenate(
            [x[block * groups : (block + 1) * groups].astype(F32) for x in mixed], axis=0
        ).astype(BF16)
        moved = matmul(rows, move)
        for k in range(2 * zones):
            at = k * 4 * groups + block * groups
            spread_ref[at : at + groups, :] = moved[k * groups : (k + 1) * groups]
    turned_ref[...] = head_ref[...].T
    fetch.wait()


def finish_kernel(count, *refs):
    pieces, refs = refs[:count], refs[count:]
    slot_ref, own_ref, chain_ref, spread_ref, start_ref, centre_ref, refs = *refs[:6], refs[6:]
    radial_refs, (contour_ref, out_ref, flat_ref) = refs[:-3], refs[-3:]
    zones = out_ref.shape[0]
    near = jnp.concatenate([ref[...] for ref in pieces], axis=0)
    far = matmul(slot_ref[...], near)
    size = own_ref.shape[0]
    weights = own_ref[...] + far[:size] + far[size:]
    per_zone = size // zones
    terms = per_zone // SUBS
    groups = weights.shape[1] // LANES
    rows = groups * SUBS
    flat_ref[...] = jnp.zeros(flat_ref.shape, F32)
    for z in range(zones):
        base = z * per_zone
        lhs = jnp.concatenate(
            [
                jnp.concatenate(
                    [
                        weights[base + p * SUBS : base + (p + 1) * SUBS, g * LANES : (g + 1) * LANES]
                        for p in range(terms)
                    ],
                    axis=1,
                )
                for g in range(groups)
            ],
            axis=0,
        )
        both = matmul(
            jnp.concatenate(split(lhs), axis=0),
            chain_ref[z * terms * LANES : (z + 1) * terms * LANES, :],
        )
        sums = both[:rows] + both[rows:] + start_ref[z * rows : (z + 1) * rows, :]
        turned = jnp.concatenate(
            [sums] + [pltpu.roll(sums, LANES - 32 * k, 1) for k in range(1, 4)], axis=0
        )
        spread = spread_ref[2 * z * 4 * groups : 2 * (z + 1) * 4 * groups, :].astype(BF16)
        change = matmul(spread, jnp.concatenate(split(turned), axis=1))
        change = change[:, :LANES] + change[:, LANES:]
        change = change[: 4 * groups] + change[4 * groups :]
        own_lanes = iota(change.shape, 0) // groups == iota(change.shape, 1) // 32
        change = jnp.where(own_lanes, change, 0.0)
        central = centre_ref[z * groups : (z + 1) * groups, :]
        for block in range(4):
            central = central + change[block * groups : (block + 1) * groups]
        for g in range(groups):
            flat_ref[z : z + 1, g * LANES : (g + 1) * LANES] = central[g : g + 1]
    central = flat_ref[...].astype(BF16)
    scale = contour_ref[0]
    at = 0
    for ref, side in zip(radial_refs, (0, 1)):
        part = scale * matmul(central, ref[...], ((1,), (side,)))
        out_ref[:, at : at + part.shape[1]] = part[:zones].astype(BF16)
        at += part.shape[1]


def vmem():
    return pl.BlockSpec(memory_space=pltpu.VMEM)


def sum_over(value, axis):
    size = lax.axis_size(axis)
    if size & (size - 1):
        return lax.psum(value.astype(F32), axis)
    stride = 1
    while stride < size:
        value = value.astype(BF16)
        radix = min(4, size // stride)
        parts = {0: value}
        for k in (3, 2, 1):
            if k < radix:
                parts[k] = lax.ppermute(value, axis, [(i, i ^ (stride * k)) for i in range(size)])
        parts = [parts[k].astype(F32) for k in range(radix)]
        value = (parts[0] + parts[1]) + (parts[2] + parts[3]) if radix == 4 else parts[0] + parts[1]
        stride *= radix
    return value


def shards(
    single_site, coupling, angular, phases, contour, radial, neighbours, owner_row, old_potential
):
    site = single_site[0]
    _, width = site.shape
    count, zones, places = neighbours.shape
    terms = angular.shape[0]
    atoms = owner_row.shape[0]
    assert atoms <= 65536 and places <= LANES and zones == 2
    assert count > 2 * REACH and sorted(SHIFTS) == [k for k in range(-REACH, REACH + 1) if k]
    assert width == 1024 and terms == 4 and atoms % LANES == 0 and places % 2 == 1
    table = owner_row.reshape(atoms // LANES, LANES)
    sources = [neighbours, table, site, coupling, angular, phases]
    hbm = pl.BlockSpec(memory_space=pltpu.HBM)
    params = pltpu.CompilerParams(vmem_limit_bytes=LIMIT)
    turned = pltpu.with_memory_space_constraint(radial[0].T, pltpu.HBM)
    parts = [HEAD * LANES, radial.shape[2] - HEAD * LANES]
    results = pl.pallas_call(
        functools.partial(pack_kernel, "dom", len(sources)),
        out_shape=[pltpu.VMEM(x.shape, x.dtype) for x in sources]
        + [pltpu.VMEM((parts[0], width), BF16)]
        + [pltpu.VMEM((CAP, width), BF16)] * len(SHIFTS),
        in_specs=[hbm] * (len(sources) + 1),
        out_specs=[vmem()] * (len(sources) + 1 + len(SHIFTS)),
        scratch_shapes=[
            pltpu.VMEM((len(SHIFTS) * zones, LANES), jnp.int32),
            pltpu.SemaphoreType.DMA((len(sources) + 1,)),
        ],
        compiler_params=params,
        name="pack",
    )(*[pltpu.with_memory_space_constraint(x, pltpu.HBM) for x in sources], turned)
    kept, head, packs = results[: len(sources)], results[len(sources)], results[len(sources) + 1 :]
    pieces = [
        lax.ppermute(pack, "dom", [(i, (i + shift) % count) for i in range(count)])
        for pack, shift in zip(packs, SHIFTS)
    ]
    size = zones * terms * SUBS
    groups = width // LANES
    prepared = pl.pallas_call(
        functools.partial(prepare_kernel, "dom", parts[0]),
        out_shape=[
            pltpu.VMEM((2 * size, CAP * len(SHIFTS)), BF16),
            pltpu.VMEM((size, width), F32),
            pltpu.VMEM((zones * terms * LANES, LANES), BF16),
            pltpu.VMEM((2 * zones * 4 * groups, 2 * LANES), F32),
            pltpu.VMEM((zones * groups * SUBS, LANES), F32),
            pltpu.VMEM((zones * groups, LANES), F32),
            pltpu.VMEM((width, parts[0]), BF16),
            pltpu.VMEM((parts[1], width), BF16),
        ],
        in_specs=[vmem()] * 7 + [hbm],
        out_specs=[vmem()] * 8,
        scratch_shapes=[
            pltpu.VMEM((zones, LANES), jnp.int32),
            pltpu.VMEM((2 * zones * SUBS, LANES), F32),
            pltpu.VMEM((groups, (terms + zones) * LANES), F32),
            pltpu.SemaphoreType.DMA,
        ],
        compiler_params=params,
        name="prepare",
    )(*kept, head, turned)
    pieces = [pltpu.with_memory_space_constraint(piece, pltpu.VMEM) for piece in pieces]
    entries = radial.shape[2]
    part = pl.pallas_call(
        functools.partial(finish_kernel, len(pieces)),
        out_shape=pltpu.VMEM((zones, entries), BF16),
        in_specs=[vmem()] * (len(pieces) + 8) + [pl.BlockSpec(memory_space=pltpu.SMEM)],
        out_specs=vmem(),
        scratch_shapes=[
            pltpu.VMEM((SUBS, width), F32),
        ],
        compiler_params=params,
        name="finish",
    )(*pieces, *prepared, contour)
    density = sum_over(part, "en")
    return 0.5 * old_potential + 0.5 * density * lax.rsqrt(1.0 + density * density)


def solution(mesh):
    return jax.shard_map(
        shards,
        mesh=mesh,
        in_specs=(
            P("en", "dom", None),
            P("dom", None, None),
            P(),
            P("en", None),
            P("en"),
            P("en", None, None),
            P(),
            P(),
            P("dom", None),
        ),
        out_specs=P("dom", None),
        check_vma=False,
    )
```

```python
import functools

import jax
import jax.numpy as jnp
from jax import lax
from jax.experimental import pallas as pl
from jax.experimental.pallas import tpu as pltpu
from jax.sharding import PartitionSpec as P


REACH = 2
CAP = 48
LIMIT = 24 << 20
LANES = 128
SUBS = 8
SHIFTS = (1, 2, -2, -1)
HEAD = 24
FLOPS = 5000000000
F32 = jnp.float32
BF16 = jnp.bfloat16


def matmul(a, b, dims=((1,), (0,))):
    return lax.dot_general(a, b, (dims, ((), ())), preferred_element_type=F32)


def iota(shape, axis):
    return lax.broadcasted_iota(jnp.int32, shape, axis)


def ones_where(mask):
    return jnp.where(mask, 1.0, 0.0).astype(BF16)


def split(x):
    high = x.astype(BF16)
    return high, (x - high.astype(F32)).astype(BF16)


def load_lists(nbr_ref, pad_ref, targets):
    zones, places = nbr_ref.shape[1:]
    pad_ref[...] = jnp.full(pad_ref.shape, -1, jnp.int32)
    for k, target in enumerate(targets):
        pad_ref[k * zones : (k + 1) * zones, 0:places] = nbr_ref[target]
    return jnp.concatenate(
        [pad_ref[r : r + 1, :] for r in range(len(targets) * zones)], axis=1
    )


def resolve(atoms, table_ref, owned):
    table = table_ref[...]
    height = table.shape[0]
    both = jnp.concatenate([table & ~255, table & 255], axis=0).astype(F32)
    both = jnp.concatenate(
        [both] + [pltpu.roll(both, LANES - 32 * k, 1) for k in range(1, 4)], axis=0
    )[:, :32].astype(BF16)
    width = atoms.shape[1]
    key = ((atoms >> 5) & 3) * height + (atoms >> 7)
    hots = []
    for k in range(4):
        hot = jnp.where(iota((height, width), 0) + k * height == key, 1.0, 0.0)
        hots += [hot, hot]
    picked = matmul(both, jnp.concatenate(hots, axis=0).astype(BF16), ((0,), (0,)))
    lane_hot = iota((32, width), 0) == (atoms & 31)
    found = jnp.sum(jnp.where(lane_hot, picked, 0.0), axis=0, keepdims=True).astype(jnp.int32)
    if owned & (owned - 1) == 0:
        domain, local = found >> (owned.bit_length() - 1), found & (owned - 1)
    else:
        domain, local = found // owned, found % owned
    return jnp.where(atoms < 0, -1, domain), local


def slot_hot(masks):
    width = masks[0].shape[1]
    rows = jnp.concatenate(
        [jnp.where(mask, 1.0, 0.0) for mask in masks]
        + [jnp.zeros((SUBS - len(masks), width), F32)],
        axis=0,
    ).astype(BF16)
    earlier = ones_where(iota((width, width), 0) < iota((width, width), 1))
    rank = matmul(rows, earlier)
    slots = iota((CAP, width), 0).astype(F32)
    return [
        ones_where((rank[k : k + 1] == slots) & mask) for k, mask in enumerate(masks)
    ]


def pack_kernel(axis, inputs, *refs):
    sources, refs = refs[:inputs], refs[inputs:]
    kept, refs = refs[:inputs], refs[inputs:]
    pack_refs, (pad_ref, sems) = refs[:-2], refs[-2:]
    copies = [
        pltpu.make_async_copy(source, ref, sems.at[k])
        for k, (source, ref) in enumerate(zip(sources, kept))
    ]
    for copy in copies:
        copy.start()
    nbr_ref, table_ref, site_ref = kept[:3]
    count = nbr_ref.shape[0]
    owned = site_ref.shape[0]
    me = lax.axis_index(axis)
    copies[0].wait()
    copies[1].wait()
    atoms = load_lists(nbr_ref, pad_ref, [lax.rem(me + shift + count, count) for shift in SHIFTS])
    domain, local = resolve(atoms, table_ref, owned)
    width = atoms.shape[1] // len(SHIFTS)
    mine = domain == me
    spans = [slice(k * width, (k + 1) * width) for k in range(len(SHIFTS))]
    hots = slot_hot([mine[:, s] for s in spans])
    rows = iota((owned, width), 0)
    chosen = [
        matmul(hot, ones_where(local[:, s] == rows), ((1,), (1,))).astype(BF16)
        for hot, s in zip(hots, spans)
    ]
    copies[2].wait()
    packed = matmul(jnp.concatenate(chosen, axis=0), site_ref[...]).astype(BF16)
    for k, pack_ref in enumerate(pack_refs):
        pack_ref[...] = packed[k * CAP : (k + 1) * CAP]
    for copy in copies[3:]:
        copy.wait()


def fold_matrix():
    return ones_where(
        (iota((LANES, LANES), 0) % 32) == (iota((LANES, LANES), 1) % 32)
    )


def block_mask():
    return (iota((LANES, LANES), 0) // 32) == (iota((LANES, LANES), 1) // 32)


def strided_row(couple_ref, zone, places):
    terms, width = couple_ref.shape[1:]
    lane = iota((terms, LANES), 1)
    merged = jnp.zeros((terms, LANES), F32)
    for begin in range(0, width, LANES):
        size = min(LANES, width - begin)
        block = couple_ref[zone, :, begin : begin + size].astype(F32)
        if size < LANES:
            spare = jnp.zeros((terms, LANES - size), F32)
            block = jnp.concatenate([block, spare], axis=1)
        kept = functools.reduce(
            jnp.logical_or,
            [lane == at - begin for at in range(0, width, places) if begin <= at < begin + size],
            lane < 0,
        )
        merged = jnp.where(kept, block, merged)
    order = ones_where(
        (iota((LANES, LANES), 1) * places) % LANES == iota((LANES, LANES), 0)
    )
    return matmul(merged.astype(BF16), order)


def prepare_kernel(
    axis, begin,
    nbr_ref, table_ref, site_ref, couple_ref, angular_ref, phase_ref, radial_ref,
    slot_ref, own_ref, chain_ref, spread_ref, start_ref, centre_ref, turned_ref,
    pad_ref, scaled_ref, grid_ref,
):
    count, zones, places = nbr_ref.shape
    owned = site_ref.shape[0]
    terms = angular_ref.shape[0]
    groups = angular_ref.shape[1] // LANES
    me = lax.axis_index(axis)
    atoms = load_lists(nbr_ref, pad_ref, [me])
    domain, local = resolve(atoms, table_ref, owned)
    width = atoms.shape[1]
    hots = slot_hot(
        [domain == lax.rem(me - shift + count, count) for shift in SHIFTS]
    )
    scaled_ref[...] = jnp.zeros(scaled_ref.shape, F32)
    lasts = [strided_row(couple_ref, z, places) for z in range(zones)]
    for z in range(zones):
        for q in range(terms):
            phase = phase_ref[0:1, q : q + 1]
            for half, rows in enumerate((couple_ref[z, :, 0:places].astype(F32), lasts[z])):
                row = (phase * rows[q : q + 1, 0:places]).astype(BF16)
                at = half * zones * SUBS + z * SUBS + q
                scaled_ref[at : at + 1, 0:places] = row.astype(F32)
    coefs = []
    for z in range(zones):
        to_first = scaled_ref[z * SUBS : (z + 1) * SUBS, :]
        at = (zones + z) * SUBS
        rows = jnp.concatenate(
            [scaled_ref[at + p : at + p + 1, :] * to_first for p in range(terms)], axis=0
        )
        blank = jnp.zeros(rows.shape, F32)
        coefs.append(
            jnp.concatenate([rows if y == z else blank for y in range(zones)], axis=1)
        )
    high, low = split(jnp.concatenate(coefs, axis=0))
    size = high.shape[0]
    both = jnp.concatenate([high, low], axis=0)
    slot_ref[...] = matmul(both, jnp.concatenate(hots, axis=0), ((1,), (1,))).astype(BF16)
    centres = ones_where(
        iota((2 * SUBS, width), 1) == iota((2 * SUBS, width), 0) * LANES
    )
    own_hot = ones_where(
        (local == iota((owned, width), 0)) & (domain == me)
    )
    own_coefs = matmul(jnp.concatenate([both, centres], axis=0), own_hot, ((1,), (1,)))
    own = matmul(own_coefs.astype(BF16), site_ref[...])
    own_ref[...] = own[:size] + own[size : 2 * size]
    centre = own[2 * size : 2 * size + zones]

    for g in range(groups):
        at = slice(g * LANES, (g + 1) * LANES)
        for q in range(terms):
            grid_ref[g : g + 1, q * LANES : (q + 1) * LANES] = angular_ref[q : q + 1, at].astype(F32)
        for z in range(zones):
            m = terms + z
            grid_ref[g : g + 1, m * LANES : (m + 1) * LANES] = centre[z : z + 1, at]
    grid = grid_ref[...]
    for z in range(zones):
        m = terms + z
        centre_ref[z * groups : (z + 1) * groups, :] = grid[:, m * LANES : (m + 1) * LANES]
        start_ref[z * groups * SUBS : (z + 1) * groups * SUBS, :] = jnp.concatenate(
            [
                scaled_ref[z * SUBS : (z + 1) * SUBS, 0:1] * grid[g : g + 1, m * LANES : (m + 1) * LANES]
                for g in range(groups)
            ],
            axis=0,
        )
    repeat = ones_where(iota((32, groups), 0) // 4 == iota((32, groups), 1))
    tall = matmul(repeat, grid.astype(BF16))
    keep = iota((32, LANES), 0) % 4 == iota((32, LANES), 1) // 32
    masked = jnp.concatenate(
        [
            jnp.where(keep, tall[:, m * LANES : (m + 1) * LANES], 0.0)
            for m in range(terms + zones)
        ],
        axis=0,
    ).astype(BF16)
    tiled = matmul(masked, fold_matrix())
    diagonal = block_mask()
    tables = tiled[: terms * 32]
    first_only = jnp.where(iota(tables.shape, 1) < 32, tables, 0.0).astype(BF16)
    for z in range(zones):
        m = terms + z
        block = tiled[m * 32 : (m + 1) * 32].astype(BF16)
        product = matmul(first_only, jnp.concatenate([block] * 4, axis=0))
        for p in range(terms):
            piece = product[p * 32 : (p + 1) * 32]
            at = (z * terms + p) * LANES
            chain_ref[at : at + LANES, :] = jnp.where(
                diagonal, jnp.concatenate([piece] * 4, axis=0), 0.0
            ).astype(BF16)
    lane_term = iota((32, LANES), 1) // 32
    side = sum(
        jnp.where(lane_term == q, tables[q * 32 : (q + 1) * 32], 0.0) for q in range(terms)
    ).astype(BF16)
    order = ones_where(
        iota((32, 32), 1) == (iota((32, 32), 0) % groups) * 4 + iota((32, 32), 0) // groups
    )
    mixed = []
    for z in range(zones):
        block = tiled[(terms + z) * 32 : (terms + z + 1) * 32].astype(BF16)
        sorted_rows = matmul(order, block).astype(BF16)
        mixed += split(matmul(sorted_rows[:, :32], side))
    row = iota((LANES, 2 * LANES), 0)
    column = iota((LANES, 2 * LANES), 1)
    same = (column % SUBS == row // 32) & ((column % 64) // SUBS == (row % 32) // 4)
    for block in range(4):
        move = ones_where(same & (row % 4 == (column // 64 + block) % 4))
        rows = jnp.concatenate(
            [x[block * groups : (block + 1) * groups].astype(F32) for x in mixed], axis=0
        ).astype(BF16)
        moved = matmul(rows, move)
        for k in range(2 * zones):
            at = k * 4 * groups + block * groups
            spread_ref[at : at + groups, :] = moved[k * groups : (k + 1) * groups]
    turned_ref[...] = radial_ref[:begin, :].T


def finish_kernel(count, *refs):
    pieces, refs = refs[:count], refs[count:]
    slot_ref, own_ref, chain_ref, spread_ref, start_ref, centre_ref, refs = *refs[:6], refs[6:]
    radial_refs, (contour_ref, out_ref, flat_ref) = refs[:-3], refs[-3:]
    zones = out_ref.shape[0]
    near = jnp.concatenate([ref[...] for ref in pieces], axis=0)
    far = matmul(slot_ref[...], near)
    size = own_ref.shape[0]
    weights = own_ref[...] + far[:size] + far[size:]
    per_zone = size // zones
    terms = per_zone // SUBS
    groups = weights.shape[1] // LANES
    rows = groups * SUBS
    flat_ref[...] = jnp.zeros(flat_ref.shape, F32)
    for z in range(zones):
        base = z * per_zone
        lhs = jnp.concatenate(
            [
                jnp.concatenate(
                    [
                        weights[base + p * SUBS : base + (p + 1) * SUBS, g * LANES : (g + 1) * LANES]
                        for p in range(terms)
                    ],
                    axis=1,
                )
                for g in range(groups)
            ],
            axis=0,
        )
        both = matmul(
            jnp.concatenate(split(lhs), axis=0),
            chain_ref[z * terms * LANES : (z + 1) * terms * LANES, :],
        )
        sums = both[:rows] + both[rows:] + start_ref[z * rows : (z + 1) * rows, :]
        turned = jnp.concatenate(
            [sums] + [pltpu.roll(sums, LANES - 32 * k, 1) for k in range(1, 4)], axis=0
        )
        spread = spread_ref[2 * z * 4 * groups : 2 * (z + 1) * 4 * groups, :].astype(BF16)
        change = matmul(spread, jnp.concatenate(split(turned), axis=1))
        change = change[:, :LANES] + change[:, LANES:]
        change = change[: 4 * groups] + change[4 * groups :]
        own_lanes = iota(change.shape, 0) // groups == iota(change.shape, 1) // 32
        change = jnp.where(own_lanes, change, 0.0)
        central = centre_ref[z * groups : (z + 1) * groups, :]
        for block in range(4):
            central = central + change[block * groups : (block + 1) * groups]
        for g in range(groups):
            flat_ref[z : z + 1, g * LANES : (g + 1) * LANES] = central[g : g + 1]
    central = flat_ref[...].astype(BF16)
    scale = contour_ref[0]
    at = 0
    turned_ref, radial_ref = radial_refs
    for matrix, side in ((turned_ref[...], 0), (radial_ref[turned_ref.shape[1] :, :], 1)):
        part = scale * matmul(central, matrix, ((1,), (side,)))
        out_ref[:, at : at + part.shape[1]] = part[:zones].astype(BF16)
        at += part.shape[1]


def vmem():
    return pl.BlockSpec(memory_space=pltpu.VMEM)


def sum_over(value, axis):
    size = lax.axis_size(axis)
    if size & (size - 1):
        return lax.psum(value.astype(F32), axis)
    stride = 1
    while stride < size:
        value = value.astype(BF16)
        radix = min(4, size // stride)
        parts = {0: value}
        for k in (3, 2, 1):
            if k < radix:
                parts[k] = lax.ppermute(value, axis, [(i, i ^ (stride * k)) for i in range(size)])
        parts = [parts[k].astype(F32) for k in range(radix)]
        value = (parts[0] + parts[1]) + (parts[2] + parts[3]) if radix == 4 else parts[0] + parts[1]
        stride *= radix
    return value


def shards(
    single_site, coupling, angular, phases, contour, radial, neighbours, owner_row, old_potential
):
    site = single_site[0]
    _, width = site.shape
    count, zones, places = neighbours.shape
    terms = angular.shape[0]
    atoms = owner_row.shape[0]
    assert atoms <= 65536 and places <= LANES and zones == 2
    assert count > 2 * REACH and sorted(SHIFTS) == [k for k in range(-REACH, REACH + 1) if k]
    assert width == 1024 and terms == 4 and atoms % LANES == 0 and places % 2 == 1
    table = owner_row.reshape(atoms // LANES, LANES)
    sources = [neighbours, table, site, coupling, angular, phases]
    hbm = pl.BlockSpec(memory_space=pltpu.HBM)
    params = pltpu.CompilerParams(vmem_limit_bytes=LIMIT)
    turned = radial[0].T
    parts = [HEAD * LANES, radial.shape[2] - HEAD * LANES]
    results = pl.pallas_call(
        functools.partial(pack_kernel, "dom", len(sources)),
        out_shape=[pltpu.VMEM(x.shape, x.dtype) for x in sources]
        + [pltpu.VMEM((CAP, width), BF16)] * len(SHIFTS),
        in_specs=[hbm] * len(sources),
        out_specs=[vmem()] * (len(sources) + len(SHIFTS)),
        scratch_shapes=[
            pltpu.VMEM((len(SHIFTS) * zones, LANES), jnp.int32),
            pltpu.SemaphoreType.DMA((len(sources),)),
        ],
        compiler_params=params,
        cost_estimate=pl.CostEstimate(flops=FLOPS, bytes_accessed=0, transcendentals=0),
        name="pack",
    )(*[pltpu.with_memory_space_constraint(x, pltpu.HBM) for x in sources])
    kept, packs = results[: len(sources)], results[len(sources) :]
    pieces = [
        lax.ppermute(pack, "dom", [(i, (i + shift) % count) for i in range(count)])
        for pack, shift in zip(packs, SHIFTS)
    ]
    size = zones * terms * SUBS
    groups = width // LANES
    prepared = pl.pallas_call(
        functools.partial(prepare_kernel, "dom", parts[0]),
        out_shape=[
            pltpu.VMEM((2 * size, CAP * len(SHIFTS)), BF16),
            pltpu.VMEM((size, width), F32),
            pltpu.VMEM((zones * terms * LANES, LANES), BF16),
            pltpu.VMEM((2 * zones * 4 * groups, 2 * LANES), F32),
            pltpu.VMEM((zones * groups * SUBS, LANES), F32),
            pltpu.VMEM((zones * groups, LANES), F32),
            pltpu.VMEM((width, parts[0]), BF16),
        ],
        in_specs=[vmem()] * 7,
        out_specs=[vmem()] * 7,
        scratch_shapes=[
            pltpu.VMEM((zones, LANES), jnp.int32),
            pltpu.VMEM((2 * zones * SUBS, LANES), F32),
            pltpu.VMEM((groups, (terms + zones) * LANES), F32),
        ],
        compiler_params=params,
        name="prepare",
    )(*kept, turned)
    pieces = [pltpu.with_memory_space_constraint(piece, pltpu.VMEM) for piece in pieces]
    entries = radial.shape[2]
    part = pl.pallas_call(
        functools.partial(finish_kernel, len(pieces)),
        out_shape=pltpu.VMEM((zones, entries), BF16),
        in_specs=[vmem()] * (len(pieces) + 8) + [pl.BlockSpec(memory_space=pltpu.SMEM)],
        out_specs=vmem(),
        scratch_shapes=[
            pltpu.VMEM((SUBS, width), F32),
        ],
        compiler_params=params,
        name="finish",
    )(*pieces, *prepared, turned, contour)
    density = sum_over(part, "en")
    return 0.5 * old_potential + 0.5 * density * lax.rsqrt(1.0 + density * density)


def solution(mesh):
    return jax.shard_map(
        shards,
        mesh=mesh,
        in_specs=(
            P("en", "dom", None),
            P("dom", None, None),
            P(),
            P("en", None),
            P("en"),
            P("en", None, None),
            P(),
            P(),
            P("dom", None),
        ),
        out_specs=P("dom", None),
        check_vma=False,
    )
```

```python
import functools

import jax
import jax.numpy as jnp
from jax import lax
from jax.experimental import pallas as pl
from jax.experimental.pallas import tpu as pltpu
from jax.sharding import PartitionSpec as P


REACH = 2
CAP = 48
LIMIT = 24 << 20
LANES = 128
SUBS = 8
SHIFTS = (1, 2, -2, -1)
FLOPS = 5000000000
F32 = jnp.float32
BF16 = jnp.bfloat16


def matmul(a, b, dims=((1,), (0,))):
    return lax.dot_general(a, b, (dims, ((), ())), preferred_element_type=F32)


def iota(shape, axis):
    return lax.broadcasted_iota(jnp.int32, shape, axis)


def ones_where(mask):
    return jnp.where(mask, 1.0, 0.0).astype(BF16)


def split(x):
    high = x.astype(BF16)
    return high, (x - high.astype(F32)).astype(BF16)


def load_lists(nbr_ref, pad_ref, targets):
    zones, places = nbr_ref.shape[1:]
    pad_ref[...] = jnp.full(pad_ref.shape, -1, jnp.int32)
    for k, target in enumerate(targets):
        pad_ref[k * zones : (k + 1) * zones, 0:places] = nbr_ref[target]
    return jnp.concatenate(
        [pad_ref[r : r + 1, :] for r in range(len(targets) * zones)], axis=1
    )


def resolve(atoms, table_ref, owned):
    table = table_ref[...]
    height = table.shape[0]
    both = jnp.concatenate([table & ~255, table & 255], axis=0).astype(F32)
    both = jnp.concatenate(
        [both] + [pltpu.roll(both, LANES - 32 * k, 1) for k in range(1, 4)], axis=0
    )[:, :32].astype(BF16)
    width = atoms.shape[1]
    key = ((atoms >> 5) & 3) * height + (atoms >> 7)
    hots = []
    for k in range(4):
        hot = jnp.where(iota((height, width), 0) + k * height == key, 1.0, 0.0)
        hots += [hot, hot]
    picked = matmul(both, jnp.concatenate(hots, axis=0).astype(BF16), ((0,), (0,)))
    lane_hot = iota((32, width), 0) == (atoms & 31)
    found = jnp.sum(jnp.where(lane_hot, picked, 0.0), axis=0, keepdims=True).astype(jnp.int32)
    if owned & (owned - 1) == 0:
        domain, local = found >> (owned.bit_length() - 1), found & (owned - 1)
    else:
        domain, local = found // owned, found % owned
    return jnp.where(atoms < 0, -1, domain), local


def slot_hot(masks):
    width = masks[0].shape[1]
    rows = jnp.concatenate(
        [jnp.where(mask, 1.0, 0.0) for mask in masks]
        + [jnp.zeros((SUBS - len(masks), width), F32)],
        axis=0,
    ).astype(BF16)
    earlier = ones_where(iota((width, width), 0) < iota((width, width), 1))
    rank = matmul(rows, earlier)
    slots = iota((CAP, width), 0).astype(F32)
    return [
        ones_where((rank[k : k + 1] == slots) & mask) for k, mask in enumerate(masks)
    ]


def pack_kernel(axis, inputs, *refs):
    sources, refs = refs[:inputs], refs[inputs:]
    kept, refs = refs[:inputs], refs[inputs:]
    pack_refs, (pad_ref, sems) = refs[:-2], refs[-2:]
    copies = [
        pltpu.make_async_copy(source, ref, sems.at[k])
        for k, (source, ref) in enumerate(zip(sources, kept))
    ]
    for copy in copies:
        copy.start()
    nbr_ref, table_ref, site_ref = kept[:3]
    count = nbr_ref.shape[0]
    owned = site_ref.shape[0]
    me = lax.axis_index(axis)
    copies[0].wait()
    copies[1].wait()
    atoms = load_lists(nbr_ref, pad_ref, [lax.rem(me + shift + count, count) for shift in SHIFTS])
    domain, local = resolve(atoms, table_ref, owned)
    width = atoms.shape[1] // len(SHIFTS)
    mine = domain == me
    spans = [slice(k * width, (k + 1) * width) for k in range(len(SHIFTS))]
    hots = slot_hot([mine[:, s] for s in spans])
    rows = iota((owned, width), 0)
    chosen = [
        matmul(hot, ones_where(local[:, s] == rows), ((1,), (1,))).astype(BF16)
        for hot, s in zip(hots, spans)
    ]
    copies[2].wait()
    packed = matmul(jnp.concatenate(chosen, axis=0), site_ref[...]).astype(BF16)
    for k, pack_ref in enumerate(pack_refs):
        pack_ref[...] = packed[k * CAP : (k + 1) * CAP]
    for copy in copies[3:]:
        copy.wait()


def fold_matrix():
    return ones_where(
        (iota((LANES, LANES), 0) % 32) == (iota((LANES, LANES), 1) % 32)
    )


def block_mask():
    return (iota((LANES, LANES), 0) // 32) == (iota((LANES, LANES), 1) // 32)


def strided_row(couple_ref, zone, places):
    terms, width = couple_ref.shape[1:]
    lane = iota((terms, LANES), 1)
    merged = jnp.zeros((terms, LANES), F32)
    for begin in range(0, width, LANES):
        size = min(LANES, width - begin)
        block = couple_ref[zone, :, begin : begin + size].astype(F32)
        if size < LANES:
            spare = jnp.zeros((terms, LANES - size), F32)
            block = jnp.concatenate([block, spare], axis=1)
        kept = functools.reduce(
            jnp.logical_or,
            [lane == at - begin for at in range(0, width, places) if begin <= at < begin + size],
            lane < 0,
        )
        merged = jnp.where(kept, block, merged)
    order = ones_where(
        (iota((LANES, LANES), 1) * places) % LANES == iota((LANES, LANES), 0)
    )
    return matmul(merged.astype(BF16), order)


def prepare_kernel(
    axis,
    nbr_ref, table_ref, site_ref, couple_ref, angular_ref, phase_ref, radial_ref,
    slot_ref, own_ref, chain_ref, spread_ref, start_ref, centre_ref, turned_ref,
    pad_ref, scaled_ref, grid_ref,
):
    count, zones, places = nbr_ref.shape
    owned = site_ref.shape[0]
    terms = angular_ref.shape[0]
    groups = angular_ref.shape[1] // LANES
    me = lax.axis_index(axis)
    atoms = load_lists(nbr_ref, pad_ref, [me])
    domain, local = resolve(atoms, table_ref, owned)
    width = atoms.shape[1]
    hots = slot_hot(
        [domain == lax.rem(me - shift + count, count) for shift in SHIFTS]
    )
    scaled_ref[...] = jnp.zeros(scaled_ref.shape, F32)
    lasts = [strided_row(couple_ref, z, places) for z in range(zones)]
    for z in range(zones):
        for q in range(terms):
            phase = phase_ref[0:1, q : q + 1]
            for half, rows in enumerate((couple_ref[z, :, 0:places].astype(F32), lasts[z])):
                row = (phase * rows[q : q + 1, 0:places]).astype(BF16)
                at = half * zones * SUBS + z * SUBS + q
                scaled_ref[at : at + 1, 0:places] = row.astype(F32)
    coefs = []
    for z in range(zones):
        to_first = scaled_ref[z * SUBS : (z + 1) * SUBS, :]
        at = (zones + z) * SUBS
        rows = jnp.concatenate(
            [scaled_ref[at + p : at + p + 1, :] * to_first for p in range(terms)], axis=0
        )
        blank = jnp.zeros(rows.shape, F32)
        coefs.append(
            jnp.concatenate([rows if y == z else blank for y in range(zones)], axis=1)
        )
    high, low = split(jnp.concatenate(coefs, axis=0))
    size = high.shape[0]
    both = jnp.concatenate([high, low], axis=0)
    slot_ref[...] = matmul(both, jnp.concatenate(hots, axis=0), ((1,), (1,))).astype(BF16)
    centres = ones_where(
        iota((2 * SUBS, width), 1) == iota((2 * SUBS, width), 0) * LANES
    )
    own_hot = ones_where(
        (local == iota((owned, width), 0)) & (domain == me)
    )
    own_coefs = matmul(jnp.concatenate([both, centres], axis=0), own_hot, ((1,), (1,)))
    own = matmul(own_coefs.astype(BF16), site_ref[...])
    own_ref[...] = own[:size] + own[size : 2 * size]
    centre = own[2 * size : 2 * size + zones]

    for g in range(groups):
        at = slice(g * LANES, (g + 1) * LANES)
        for q in range(terms):
            grid_ref[g : g + 1, q * LANES : (q + 1) * LANES] = angular_ref[q : q + 1, at].astype(F32)
        for z in range(zones):
            m = terms + z
            grid_ref[g : g + 1, m * LANES : (m + 1) * LANES] = centre[z : z + 1, at]
    grid = grid_ref[...]
    for z in range(zones):
        m = terms + z
        centre_ref[z * groups : (z + 1) * groups, :] = grid[:, m * LANES : (m + 1) * LANES]
        start_ref[z * groups * SUBS : (z + 1) * groups * SUBS, :] = jnp.concatenate(
            [
                scaled_ref[z * SUBS : (z + 1) * SUBS, 0:1] * grid[g : g + 1, m * LANES : (m + 1) * LANES]
                for g in range(groups)
            ],
            axis=0,
        )
    repeat = ones_where(iota((32, groups), 0) // 4 == iota((32, groups), 1))
    tall = matmul(repeat, grid.astype(BF16))
    keep = iota((32, LANES), 0) % 4 == iota((32, LANES), 1) // 32
    masked = jnp.concatenate(
        [
            jnp.where(keep, tall[:, m * LANES : (m + 1) * LANES], 0.0)
            for m in range(terms + zones)
        ],
        axis=0,
    ).astype(BF16)
    tiled = matmul(masked, fold_matrix())
    diagonal = block_mask()
    tables = tiled[: terms * 32]
    first_only = jnp.where(iota(tables.shape, 1) < 32, tables, 0.0).astype(BF16)
    for z in range(zones):
        m = terms + z
        block = tiled[m * 32 : (m + 1) * 32].astype(BF16)
        product = matmul(first_only, jnp.concatenate([block] * 4, axis=0))
        for p in range(terms):
            piece = product[p * 32 : (p + 1) * 32]
            at = (z * terms + p) * LANES
            chain_ref[at : at + LANES, :] = jnp.where(
                diagonal, jnp.concatenate([piece] * 4, axis=0), 0.0
            ).astype(BF16)
    lane_term = iota((32, LANES), 1) // 32
    side = sum(
        jnp.where(lane_term == q, tables[q * 32 : (q + 1) * 32], 0.0) for q in range(terms)
    ).astype(BF16)
    order = ones_where(
        iota((32, 32), 1) == (iota((32, 32), 0) % groups) * 4 + iota((32, 32), 0) // groups
    )
    mixed = []
    for z in range(zones):
        block = tiled[(terms + z) * 32 : (terms + z + 1) * 32].astype(BF16)
        sorted_rows = matmul(order, block).astype(BF16)
        mixed += split(matmul(sorted_rows[:, :32], side))
    row = iota((LANES, 2 * LANES), 0)
    column = iota((LANES, 2 * LANES), 1)
    same = (column % SUBS == row // 32) & ((column % 64) // SUBS == (row % 32) // 4)
    for block in range(4):
        move = ones_where(same & (row % 4 == (column // 64 + block) % 4))
        rows = jnp.concatenate(
            [x[block * groups : (block + 1) * groups].astype(F32) for x in mixed], axis=0
        ).astype(BF16)
        moved = matmul(rows, move)
        for k in range(2 * zones):
            at = k * 4 * groups + block * groups
            spread_ref[at : at + groups, :] = moved[k * groups : (k + 1) * groups]
    turned_ref[...] = radial_ref[...].T


def finish_kernel(count, *refs):
    pieces, refs = refs[:count], refs[count:]
    slot_ref, own_ref, chain_ref, spread_ref, start_ref, centre_ref, refs = *refs[:6], refs[6:]
    turned_ref, contour_ref, out_ref, flat_ref = refs
    zones = out_ref.shape[0]
    near = jnp.concatenate([ref[...] for ref in pieces], axis=0)
    far = matmul(slot_ref[...], near)
    size = own_ref.shape[0]
    weights = own_ref[...] + far[:size] + far[size:]
    per_zone = size // zones
    terms = per_zone // SUBS
    groups = weights.shape[1] // LANES
    rows = groups * SUBS
    flat_ref[...] = jnp.zeros(flat_ref.shape, F32)
    for z in range(zones):
        base = z * per_zone
        lhs = jnp.concatenate(
            [
                jnp.concatenate(
                    [
                        weights[base + p * SUBS : base + (p + 1) * SUBS, g * LANES : (g + 1) * LANES]
                        for p in range(terms)
                    ],
                    axis=1,
                )
                for g in range(groups)
            ],
            axis=0,
        )
        both = matmul(
            jnp.concatenate(split(lhs), axis=0),
            chain_ref[z * terms * LANES : (z + 1) * terms * LANES, :],
        )
        sums = both[:rows] + both[rows:] + start_ref[z * rows : (z + 1) * rows, :]
        turned = jnp.concatenate(
            [sums] + [pltpu.roll(sums, LANES - 32 * k, 1) for k in range(1, 4)], axis=0
        )
        spread = spread_ref[2 * z * 4 * groups : 2 * (z + 1) * 4 * groups, :].astype(BF16)
        change = matmul(spread, jnp.concatenate(split(turned), axis=1))
        change = change[:, :LANES] + change[:, LANES:]
        change = change[: 4 * groups] + change[4 * groups :]
        own_lanes = iota(change.shape, 0) // groups == iota(change.shape, 1) // 32
        change = jnp.where(own_lanes, change, 0.0)
        central = centre_ref[z * groups : (z + 1) * groups, :]
        for block in range(4):
            central = central + change[block * groups : (block + 1) * groups]
        for g in range(groups):
            flat_ref[z : z + 1, g * LANES : (g + 1) * LANES] = central[g : g + 1]
    central = flat_ref[...].astype(BF16)
    scale = contour_ref[0]
    out_ref[...] = (scale * matmul(central, turned_ref[...])[:zones]).astype(BF16)


def vmem():
    return pl.BlockSpec(memory_space=pltpu.VMEM)


def sum_over(value, axis):
    size = lax.axis_size(axis)
    if size & (size - 1):
        return lax.psum(value.astype(F32), axis)
    stride = 1
    while stride < size:
        value = value.astype(BF16)
        radix = min(4, size // stride)
        parts = {0: value}
        for k in (3, 2, 1):
            if k < radix:
                parts[k] = lax.ppermute(value, axis, [(i, i ^ (stride * k)) for i in range(size)])
        parts = [parts[k].astype(F32) for k in range(radix)]
        value = (parts[0] + parts[1]) + (parts[2] + parts[3]) if radix == 4 else parts[0] + parts[1]
        stride *= radix
    return value


def shards(
    single_site, coupling, angular, phases, contour, radial, neighbours, owner_row, old_potential
):
    site = single_site[0]
    _, width = site.shape
    count, zones, places = neighbours.shape
    terms = angular.shape[0]
    atoms = owner_row.shape[0]
    assert atoms <= 65536 and places <= LANES and zones == 2
    assert count > 2 * REACH and sorted(SHIFTS) == [k for k in range(-REACH, REACH + 1) if k]
    assert width == 1024 and terms == 4 and atoms % LANES == 0 and places % 2 == 1
    table = owner_row.reshape(atoms // LANES, LANES)
    sources = [neighbours, table, site, coupling, angular, phases]
    hbm = pl.BlockSpec(memory_space=pltpu.HBM)
    params = pltpu.CompilerParams(vmem_limit_bytes=LIMIT)
    turned = radial[0].T
    results = pl.pallas_call(
        functools.partial(pack_kernel, "dom", len(sources)),
        out_shape=[pltpu.VMEM(x.shape, x.dtype) for x in sources]
        + [pltpu.VMEM((CAP, width), BF16)] * len(SHIFTS),
        in_specs=[hbm] * len(sources),
        out_specs=[vmem()] * (len(sources) + len(SHIFTS)),
        scratch_shapes=[
            pltpu.VMEM((len(SHIFTS) * zones, LANES), jnp.int32),
            pltpu.SemaphoreType.DMA((len(sources),)),
        ],
        compiler_params=params,
        cost_estimate=pl.CostEstimate(flops=FLOPS, bytes_accessed=0, transcendentals=0),
        name="pack",
    )(*[pltpu.with_memory_space_constraint(x, pltpu.HBM) for x in sources])
    kept, packs = results[: len(sources)], results[len(sources) :]
    pieces = [
        lax.ppermute(pack, "dom", [(i, (i + shift) % count) for i in range(count)])
        for pack, shift in zip(packs, SHIFTS)
    ]
    size = zones * terms * SUBS
    groups = width // LANES
    prepared = pl.pallas_call(
        functools.partial(prepare_kernel, "dom"),
        out_shape=[
            pltpu.VMEM((2 * size, CAP * len(SHIFTS)), BF16),
            pltpu.VMEM((size, width), F32),
            pltpu.VMEM((zones * terms * LANES, LANES), BF16),
            pltpu.VMEM((2 * zones * 4 * groups, 2 * LANES), F32),
            pltpu.VMEM((zones * groups * SUBS, LANES), F32),
            pltpu.VMEM((zones * groups, LANES), F32),
            pltpu.VMEM((width, radial.shape[2]), BF16),
        ],
        in_specs=[vmem()] * 7,
        out_specs=[vmem()] * 7,
        scratch_shapes=[
            pltpu.VMEM((zones, LANES), jnp.int32),
            pltpu.VMEM((2 * zones * SUBS, LANES), F32),
            pltpu.VMEM((groups, (terms + zones) * LANES), F32),
        ],
        compiler_params=params,
        name="prepare",
    )(*kept, turned)
    pieces = [pltpu.with_memory_space_constraint(piece, pltpu.VMEM) for piece in pieces]
    entries = radial.shape[2]
    part = pl.pallas_call(
        functools.partial(finish_kernel, len(pieces)),
        out_shape=pltpu.VMEM((zones, entries), BF16),
        in_specs=[vmem()] * (len(pieces) + 7) + [pl.BlockSpec(memory_space=pltpu.SMEM)],
        out_specs=vmem(),
        scratch_shapes=[
            pltpu.VMEM((SUBS, width), F32),
        ],
        compiler_params=params,
        name="finish",
    )(*pieces, *prepared, contour)
    density = sum_over(part, "en")
    return 0.5 * old_potential + 0.5 * density * lax.rsqrt(1.0 + density * density)


def solution(mesh):
    return jax.shard_map(
        shards,
        mesh=mesh,
        in_specs=(
            P("en", "dom", None),
            P("dom", None, None),
            P(),
            P("en", None),
            P("en"),
            P("en", None, None),
            P(),
            P(),
            P("dom", None),
        ),
        out_specs=P("dom", None),
        check_vma=False,
    )
```

```python
import functools

import jax
import jax.numpy as jnp
from jax import lax
from jax.experimental import pallas as pl
from jax.experimental.pallas import tpu as pltpu
from jax.sharding import PartitionSpec as P


REACH = 2
CAP = 48
LIMIT = 24 << 20
LANES = 128
SUBS = 8
SHIFTS = (1, 2, -2, -1)
FLOPS = 5000000000
F32 = jnp.float32
BF16 = jnp.bfloat16


def matmul(a, b, dims=((1,), (0,))):
    return lax.dot_general(a, b, (dims, ((), ())), preferred_element_type=F32)


def iota(shape, axis):
    return lax.broadcasted_iota(jnp.int32, shape, axis)


def ones_where(mask):
    return jnp.where(mask, 1.0, 0.0).astype(BF16)


def split(x):
    high = x.astype(BF16)
    return high, (x - high.astype(F32)).astype(BF16)


def load_lists(nbr_ref, pad_ref, targets):
    zones, places = nbr_ref.shape[1:]
    pad_ref[...] = jnp.full(pad_ref.shape, -1, jnp.int32)
    for k, target in enumerate(targets):
        pad_ref[k * zones : (k + 1) * zones, 0:places] = nbr_ref[target]
    return jnp.concatenate(
        [pad_ref[r : r + 1, :] for r in range(len(targets) * zones)], axis=1
    )


def resolve(atoms, table_ref, owned):
    table = table_ref[...]
    height = table.shape[0]
    both = jnp.concatenate([table & ~255, table & 255], axis=0).astype(F32)
    both = jnp.concatenate(
        [both] + [pltpu.roll(both, LANES - 32 * k, 1) for k in range(1, 4)], axis=0
    )[:, :32].astype(BF16)
    width = atoms.shape[1]
    key = ((atoms >> 5) & 3) * height + (atoms >> 7)
    hots = []
    for k in range(4):
        hot = jnp.where(iota((height, width), 0) + k * height == key, 1.0, 0.0)
        hots += [hot, hot]
    picked = matmul(both, jnp.concatenate(hots, axis=0).astype(BF16), ((0,), (0,)))
    lane_hot = iota((32, width), 0) == (atoms & 31)
    found = jnp.sum(jnp.where(lane_hot, picked, 0.0), axis=0, keepdims=True).astype(jnp.int32)
    if owned & (owned - 1) == 0:
        domain, local = found >> (owned.bit_length() - 1), found & (owned - 1)
    else:
        domain, local = found // owned, found % owned
    return jnp.where(atoms < 0, -1, domain), local


def slot_hot(masks):
    width = masks[0].shape[1]
    rows = jnp.concatenate(
        [jnp.where(mask, 1.0, 0.0) for mask in masks]
        + [jnp.zeros((SUBS - len(masks), width), F32)],
        axis=0,
    ).astype(BF16)
    earlier = ones_where(iota((width, width), 0) < iota((width, width), 1))
    rank = matmul(rows, earlier)
    slots = iota((CAP, width), 0).astype(F32)
    return [
        ones_where((rank[k : k + 1] == slots) & mask) for k, mask in enumerate(masks)
    ]


def pack_kernel(axis, inputs, *refs):
    sources, refs = refs[:inputs], refs[inputs:]
    kept, refs = refs[:inputs], refs[inputs:]
    pack_refs, (pad_ref, sems) = refs[:-2], refs[-2:]
    copies = [
        pltpu.make_async_copy(source, ref, sems.at[k])
        for k, (source, ref) in enumerate(zip(sources, kept))
    ]
    for copy in copies:
        copy.start()
    nbr_ref, table_ref, site_ref = kept[:3]
    count = nbr_ref.shape[0]
    owned = site_ref.shape[0]
    me = lax.axis_index(axis)
    copies[0].wait()
    copies[1].wait()
    atoms = load_lists(nbr_ref, pad_ref, [lax.rem(me + shift + count, count) for shift in SHIFTS])
    domain, local = resolve(atoms, table_ref, owned)
    width = atoms.shape[1] // len(SHIFTS)
    mine = domain == me
    spans = [slice(k * width, (k + 1) * width) for k in range(len(SHIFTS))]
    hots = slot_hot([mine[:, s] for s in spans])
    rows = iota((owned, width), 0).astype(F32).astype(BF16)
    chosen = [
        matmul(
            hot,
            jnp.where(local[:, s].astype(F32).astype(BF16) == rows, BF16(1), BF16(0)),
            ((1,), (1,)),
        ).astype(BF16)
        for hot, s in zip(hots, spans)
    ]
    copies[2].wait()
    packed = matmul(jnp.concatenate(chosen, axis=0), site_ref[...]).astype(BF16)
    for k, pack_ref in enumerate(pack_refs):
        pack_ref[...] = packed[k * CAP : (k + 1) * CAP]
    for copy in copies[3:]:
        copy.wait()


def fold_matrix():
    return ones_where(
        (iota((LANES, LANES), 0) % 32) == (iota((LANES, LANES), 1) % 32)
    )


def block_mask():
    return (iota((LANES, LANES), 0) // 32) == (iota((LANES, LANES), 1) // 32)


def strided_row(couple_ref, zone, places):
    terms, width = couple_ref.shape[1:]
    lane = iota((terms, LANES), 1)
    merged = jnp.zeros((terms, LANES), F32)
    for begin in range(0, width, LANES):
        size = min(LANES, width - begin)
        block = couple_ref[zone, :, begin : begin + size].astype(F32)
        if size < LANES:
            spare = jnp.zeros((terms, LANES - size), F32)
            block = jnp.concatenate([block, spare], axis=1)
        kept = functools.reduce(
            jnp.logical_or,
            [lane == at - begin for at in range(0, width, places) if begin <= at < begin + size],
            lane < 0,
        )
        merged = jnp.where(kept, block, merged)
    order = ones_where(
        (iota((LANES, LANES), 1) * places) % LANES == iota((LANES, LANES), 0)
    )
    return matmul(merged.astype(BF16), order)


def prepare_kernel(
    axis,
    nbr_ref, table_ref, site_ref, couple_ref, angular_ref, phase_ref, radial_ref,
    slot_ref, own_ref, chain_ref, spread_ref, start_ref, centre_ref, turned_ref,
    pad_ref, scaled_ref, grid_ref,
):
    count, zones, places = nbr_ref.shape
    owned = site_ref.shape[0]
    terms = angular_ref.shape[0]
    groups = angular_ref.shape[1] // LANES
    me = lax.axis_index(axis)
    atoms = load_lists(nbr_ref, pad_ref, [me])
    domain, local = resolve(atoms, table_ref, owned)
    width = atoms.shape[1]
    hots = slot_hot(
        [domain == lax.rem(me - shift + count, count) for shift in SHIFTS]
    )
    scaled_ref[...] = jnp.zeros(scaled_ref.shape, F32)
    lasts = [strided_row(couple_ref, z, places) for z in range(zones)]
    for z in range(zones):
        for q in range(terms):
            phase = phase_ref[0:1, q : q + 1]
            for half, rows in enumerate((couple_ref[z, :, 0:places].astype(F32), lasts[z])):
                row = (phase * rows[q : q + 1, 0:places]).astype(BF16)
                at = half * zones * SUBS + z * SUBS + q
                scaled_ref[at : at + 1, 0:places] = row.astype(F32)
    coefs = []
    for z in range(zones):
        to_first = scaled_ref[z * SUBS : (z + 1) * SUBS, :]
        at = (zones + z) * SUBS
        rows = jnp.concatenate(
            [scaled_ref[at + p : at + p + 1, :] * to_first for p in range(terms)], axis=0
        )
        blank = jnp.zeros(rows.shape, F32)
        coefs.append(
            jnp.concatenate([rows if y == z else blank for y in range(zones)], axis=1)
        )
    high, low = split(jnp.concatenate(coefs, axis=0))
    size = high.shape[0]
    both = jnp.concatenate([high, low], axis=0)
    slot_ref[...] = matmul(both, jnp.concatenate(hots, axis=0), ((1,), (1,))).astype(BF16)
    centres = ones_where(
        iota((2 * SUBS, width), 1) == iota((2 * SUBS, width), 0) * LANES
    )
    own_hot = ones_where(
        (local == iota((owned, width), 0)) & (domain == me)
    )
    own_coefs = matmul(jnp.concatenate([both, centres], axis=0), own_hot, ((1,), (1,)))
    own = matmul(own_coefs.astype(BF16), site_ref[...])
    own_ref[...] = own[:size] + own[size : 2 * size]
    centre = own[2 * size : 2 * size + zones]

    for g in range(groups):
        at = slice(g * LANES, (g + 1) * LANES)
        for q in range(terms):
            grid_ref[g : g + 1, q * LANES : (q + 1) * LANES] = angular_ref[q : q + 1, at].astype(F32)
        for z in range(zones):
            m = terms + z
            grid_ref[g : g + 1, m * LANES : (m + 1) * LANES] = centre[z : z + 1, at]
    grid = grid_ref[...]
    for z in range(zones):
        m = terms + z
        centre_ref[z * groups : (z + 1) * groups, :] = grid[:, m * LANES : (m + 1) * LANES]
        start_ref[z * groups * SUBS : (z + 1) * groups * SUBS, :] = jnp.concatenate(
            [
                scaled_ref[z * SUBS : (z + 1) * SUBS, 0:1] * grid[g : g + 1, m * LANES : (m + 1) * LANES]
                for g in range(groups)
            ],
            axis=0,
        )
    repeat = ones_where(iota((32, groups), 0) // 4 == iota((32, groups), 1))
    tall = matmul(repeat, grid.astype(BF16))
    keep = iota((32, LANES), 0) % 4 == iota((32, LANES), 1) // 32
    masked = jnp.concatenate(
        [
            jnp.where(keep, tall[:, m * LANES : (m + 1) * LANES], 0.0)
            for m in range(terms + zones)
        ],
        axis=0,
    ).astype(BF16)
    tiled = matmul(masked, fold_matrix())
    diagonal = block_mask()
    tables = tiled[: terms * 32]
    first_only = jnp.where(iota(tables.shape, 1) < 32, tables, 0.0).astype(BF16)
    for z in range(zones):
        m = terms + z
        block = tiled[m * 32 : (m + 1) * 32].astype(BF16)
        product = matmul(first_only, jnp.concatenate([block] * 4, axis=0))
        for p in range(terms):
            piece = product[p * 32 : (p + 1) * 32]
            at = (z * terms + p) * LANES
            chain_ref[at : at + LANES, :] = jnp.where(
                diagonal, jnp.concatenate([piece] * 4, axis=0), 0.0
            ).astype(BF16)
    lane_term = iota((32, LANES), 1) // 32
    side = sum(
        jnp.where(lane_term == q, tables[q * 32 : (q + 1) * 32], 0.0) for q in range(terms)
    ).astype(BF16)
    order = ones_where(
        iota((32, 32), 1) == (iota((32, 32), 0) % groups) * 4 + iota((32, 32), 0) // groups
    )
    mixed = []
    for z in range(zones):
        block = tiled[(terms + z) * 32 : (terms + z + 1) * 32].astype(BF16)
        sorted_rows = matmul(order, block).astype(BF16)
        mixed += split(matmul(sorted_rows[:, :32], side))
    row = iota((LANES, 2 * LANES), 0)
    column = iota((LANES, 2 * LANES), 1)
    same = (column % SUBS == row // 32) & ((column % 64) // SUBS == (row % 32) // 4)
    for block in range(4):
        move = ones_where(same & (row % 4 == (column // 64 + block) % 4))
        rows = jnp.concatenate(
            [x[block * groups : (block + 1) * groups].astype(F32) for x in mixed], axis=0
        ).astype(BF16)
        moved = matmul(rows, move)
        for k in range(2 * zones):
            at = k * 4 * groups + block * groups
            spread_ref[at : at + groups, :] = moved[k * groups : (k + 1) * groups]
    turned_ref[...] = radial_ref[...].T


def finish_kernel(count, *refs):
    pieces, refs = refs[:count], refs[count:]
    slot_ref, own_ref, chain_ref, spread_ref, start_ref, centre_ref, refs = *refs[:6], refs[6:]
    turned_ref, contour_ref, out_ref, flat_ref = refs
    zones = out_ref.shape[0]
    near = jnp.concatenate([ref[...] for ref in pieces], axis=0)
    far = matmul(slot_ref[...], near)
    size = own_ref.shape[0]
    weights = own_ref[...] + far[:size] + far[size:]
    per_zone = size // zones
    terms = per_zone // SUBS
    groups = weights.shape[1] // LANES
    rows = groups * SUBS
    flat_ref[...] = jnp.zeros(flat_ref.shape, F32)
    for z in range(zones):
        base = z * per_zone
        lhs = jnp.concatenate(
            [
                jnp.concatenate(
                    [
                        weights[base + p * SUBS : base + (p + 1) * SUBS, g * LANES : (g + 1) * LANES]
                        for p in range(terms)
                    ],
                    axis=1,
                )
                for g in range(groups)
            ],
            axis=0,
        )
        both = matmul(
            jnp.concatenate(split(lhs), axis=0),
            chain_ref[z * terms * LANES : (z + 1) * terms * LANES, :],
        )
        sums = both[:rows] + both[rows:] + start_ref[z * rows : (z + 1) * rows, :]
        turned = jnp.concatenate(
            [sums] + [pltpu.roll(sums, LANES - 32 * k, 1) for k in range(1, 4)], axis=0
        )
        spread = spread_ref[2 * z * 4 * groups : 2 * (z + 1) * 4 * groups, :].astype(BF16)
        change = matmul(spread, jnp.concatenate(split(turned), axis=1))
        change = change[:, :LANES] + change[:, LANES:]
        change = change[: 4 * groups] + change[4 * groups :]
        own_lanes = iota(change.shape, 0) // groups == iota(change.shape, 1) // 32
        change = jnp.where(own_lanes, change, 0.0)
        central = centre_ref[z * groups : (z + 1) * groups, :]
        for block in range(4):
            central = central + change[block * groups : (block + 1) * groups]
        for g in range(groups):
            flat_ref[z : z + 1, g * LANES : (g + 1) * LANES] = central[g : g + 1]
    central = flat_ref[...].astype(BF16)
    scale = contour_ref[0]
    out_ref[...] = (scale * matmul(central, turned_ref[...])[:zones]).astype(BF16)


def vmem():
    return pl.BlockSpec(memory_space=pltpu.VMEM)


def sum_over(value, axis):
    size = lax.axis_size(axis)
    if size & (size - 1):
        return lax.psum(value.astype(F32), axis)
    stride = 1
    while stride < size:
        value = value.astype(BF16)
        radix = min(4, size // stride)
        parts = {0: value}
        for k in (3, 2, 1):
            if k < radix:
                parts[k] = lax.ppermute(value, axis, [(i, i ^ (stride * k)) for i in range(size)])
        parts = [parts[k].astype(F32) for k in range(radix)]
        value = (parts[0] + parts[1]) + (parts[2] + parts[3]) if radix == 4 else parts[0] + parts[1]
        stride *= radix
    return value


def shards(
    single_site, coupling, angular, phases, contour, radial, neighbours, owner_row, old_potential
):
    site = single_site[0]
    owned, width = site.shape
    count, zones, places = neighbours.shape
    terms = angular.shape[0]
    atoms = owner_row.shape[0]
    assert owned <= 256 and atoms <= 65536 and places <= LANES and zones == 2
    assert count > 2 * REACH and sorted(SHIFTS) == [k for k in range(-REACH, REACH + 1) if k]
    assert width == 1024 and terms == 4 and atoms % LANES == 0 and places % 2 == 1
    table = owner_row.reshape(atoms // LANES, LANES)
    sources = [neighbours, table, site, coupling, angular, phases]
    hbm = pl.BlockSpec(memory_space=pltpu.HBM)
    params = pltpu.CompilerParams(vmem_limit_bytes=LIMIT)
    turned = radial[0].T
    results = pl.pallas_call(
        functools.partial(pack_kernel, "dom", len(sources)),
        out_shape=[pltpu.VMEM(x.shape, x.dtype) for x in sources]
        + [pltpu.VMEM((CAP, width), BF16)] * len(SHIFTS),
        in_specs=[hbm] * len(sources),
        out_specs=[vmem()] * (len(sources) + len(SHIFTS)),
        scratch_shapes=[
            pltpu.VMEM((len(SHIFTS) * zones, LANES), jnp.int32),
            pltpu.SemaphoreType.DMA((len(sources),)),
        ],
        compiler_params=params,
        cost_estimate=pl.CostEstimate(flops=FLOPS, bytes_accessed=0, transcendentals=0),
        name="pack",
    )(*[pltpu.with_memory_space_constraint(x, pltpu.HBM) for x in sources])
    kept, packs = results[: len(sources)], results[len(sources) :]
    pieces = [
        lax.ppermute(pack, "dom", [(i, (i + shift) % count) for i in range(count)])
        for pack, shift in zip(packs, SHIFTS)
    ]
    size = zones * terms * SUBS
    groups = width // LANES
    prepared = pl.pallas_call(
        functools.partial(prepare_kernel, "dom"),
        out_shape=[
            pltpu.VMEM((2 * size, CAP * len(SHIFTS)), BF16),
            pltpu.VMEM((size, width), F32),
            pltpu.VMEM((zones * terms * LANES, LANES), BF16),
            pltpu.VMEM((2 * zones * 4 * groups, 2 * LANES), F32),
            pltpu.VMEM((zones * groups * SUBS, LANES), F32),
            pltpu.VMEM((zones * groups, LANES), F32),
            pltpu.VMEM((width, radial.shape[2]), BF16),
        ],
        in_specs=[vmem()] * 7,
        out_specs=[vmem()] * 7,
        scratch_shapes=[
            pltpu.VMEM((zones, LANES), jnp.int32),
            pltpu.VMEM((2 * zones * SUBS, LANES), F32),
            pltpu.VMEM((groups, (terms + zones) * LANES), F32),
        ],
        compiler_params=params,
        name="prepare",
    )(*kept, turned)
    pieces = [pltpu.with_memory_space_constraint(piece, pltpu.VMEM) for piece in pieces]
    entries = radial.shape[2]
    part = pl.pallas_call(
        functools.partial(finish_kernel, len(pieces)),
        out_shape=pltpu.VMEM((zones, entries), BF16),
        in_specs=[vmem()] * (len(pieces) + 7) + [pl.BlockSpec(memory_space=pltpu.SMEM)],
        out_specs=vmem(),
        scratch_shapes=[
            pltpu.VMEM((SUBS, width), F32),
        ],
        compiler_params=params,
        name="finish",
    )(*pieces, *prepared, contour)
    density = sum_over(part, "en")
    return 0.5 * old_potential + 0.5 * density * lax.rsqrt(1.0 + density * density)


def solution(mesh):
    return jax.shard_map(
        shards,
        mesh=mesh,
        in_specs=(
            P("en", "dom", None),
            P("dom", None, None),
            P(),
            P("en", None),
            P("en"),
            P("en", None, None),
            P(),
            P(),
            P("dom", None),
        ),
        out_specs=P("dom", None),
        check_vma=False,
    )
```
